32 devices in a mesh: groups: 2 (over y), blk: 4 (over z), desc: 2 (over x), half: 2 (over core).
Axes of the slice: x: 2, y: 2, z: 4, core: 2. Of those that a mesh axis runs over, the one named last changes fastest.
Arguments:
- descriptors: bfloat16 [8, 2048, 128], P(('groups', 'blk'), ('desc', 'half')), parts along dimension 0, may hold values from -0.5 to 0.5
Outputs:
- best_dist: float32 [3, 8, 2048], P(None, ('groups', 'blk'), 'desc'), parts along dimension 1
- second_dist: float32 [3, 8, 2048], P(None, ('groups', 'blk'), 'desc'), parts along dimension 1
The draws below stay inside these ranges and needn't reach their ends.
There are 2 independent parts, one for each index of `groups`. The reference program is written for one: setup_inputs(seed, part) draws one part's arguments, and reference() takes and returns one part's arrays. A program takes and returns all parts, laid end to end along the dimension named above; each array names one. Nothing has to cross between parts.
All inputs are finite; a program needn't handle non-finite values.
Results may differ from the reference program's by a relative error of at most 0.0003.
Values may be sent and summed in bfloat16 or wider, within the bound.
A program may use at most 64 MiB of HBM per device.

```python
import jax
import jax.numpy as jnp
from jax import lax

DESC = 2048
DIM = 128
IMAGES = 4


def block_levels(stream_key, extent, split, least, high):
    def one(position, parts):
        steps = jax.random.uniform(jax.random.fold_in(jax.random.fold_in(stream_key, 6), position), (parts,), jnp.float32, least / len(split), high / len(split))
        return jnp.repeat(jnp.exp(steps), extent[position] // parts).reshape((-1,) + (1,) * (len(extent) - position - 1))

    gain = one(*split[0])
    for cut in split[1:]:
        gain = gain * one(*cut)
    return gain


def bell_draw(own_key, extent, width, limit, shards=(), kind=jnp.bfloat16):
    values = jax.random.normal(own_key, extent, jnp.float32) * width
    if len(shards) > 0:
        values = block_levels(own_key, extent, shards, -0.22, 0.18) * values
    return jnp.clip(values, min=-limit, max=limit).astype(kind)


def setup_inputs(seed: int = 0, part: int = 0) -> dict:
    seeds = jax.random.split(jax.random.key(seed), 2)
    part_keys = jax.random.split(jax.random.fold_in(seeds[1], part), 2)
    descriptors = bell_draw(part_keys[0], (IMAGES, DESC, DIM), DIM ** -0.5, 0.5, ((0, 4), (1, 4)))
    return {"descriptors": descriptors}


def reference(descriptors):
    widened = descriptors.astype(jnp.float32)
    all_norms = jnp.sum(widened * widened, axis=2)

    def per_image(entry):
        image_rows, row_norms = entry
        products = jnp.einsum("rk,jck->jrc", image_rows, widened, precision=lax.Precision.HIGHEST)
        partial_value = all_norms[:, None, :] - 2.0 * products
        negated, unused = lax.top_k(-partial_value, 2)
        return row_norms[None, :] - negated[..., 0], row_norms[None, :] - negated[..., 1]

    best_all, second_all = lax.map(per_image, (widened, all_norms))
    query_index = jnp.arange(IMAGES, dtype=jnp.int32)
    offsets = jnp.arange(1, IMAGES, dtype=jnp.int32)
    cand_index = (query_index[None, :] - offsets[:, None]) % IMAGES
    best_dist = best_all[query_index[None, :], cand_index]
    second_dist = second_all[query_index[None, :], cand_index]
    return best_dist, second_dist
```

```python
import functools

import jax
import jax.numpy as jnp
from jax import lax
from jax.experimental import pallas as pl
from jax.experimental.pallas import tpu as pltpu
from jax.sharding import PartitionSpec as P

MESH = pl.DeviceIdType.MESH


def combine(lo_a, se_a, lo_b, se_b):
    return (
        jnp.minimum(lo_a, lo_b),
        jnp.minimum(jnp.maximum(lo_a, lo_b), jnp.minimum(se_a, se_b)),
    )


def nt_dot(a, b):
    return lax.dot_general(a, b, (((1,), (1,)), ((), ())), preferred_element_type=jnp.float32)


def fold(part, lo, se):
    for r in range(part.shape[0] // 8):
        value = part[8 * r : 8 * r + 8]
        se = jnp.minimum(se, jnp.maximum(lo, value))
        lo = jnp.minimum(lo, value)
    return lo, se


def across_rows(lo, se):
    for turn in (4, 2, 1):
        lo, se = combine(lo, se, pltpu.roll(lo, turn, 0), pltpu.roll(se, turn, 0))
    return lo[0:1], se[0:1]


def kernel(
    n, D, H, CH, x_hbm, best_ref, second_ref, norm_ref,
    x_ref, buf, q, sn, low, sec, mine, inbox, turned, returned,
    x_sem, go, z_send, z_recv, q_send, q_recv, p_send, p_recv, m_send, m_recv,
):
    R = x_hbm.shape[0]
    load = pltpu.make_async_copy(x_hbm, x_ref, x_sem)
    load.start()
    CR = R // CH
    share = H * R
    Q = D * share
    TQ = min(256, share)
    T = n // 2
    i = lax.axis_index("blk")
    d = lax.axis_index("desc")
    h = lax.axis_index("half")
    others = [(dd, hh) for dd in range(D) for hh in range(H) if (dd, hh) != (0, 0)]

    if n % 2 == 0:
        hosts_tie = (i < T) == (lax.rem(lax.rem(i, T), 2) == 0)
    else:
        hosts_tie = i >= 0

    def hosting(s):
        return (2 * s != n) | hosts_tie

    def visiting(s):
        if n % 2 == 0:
            return (2 * s != n) | jnp.logical_not(hosts_tie)
        return 2 * s != n

    def guest_of(s):
        return lax.rem(i - s + n, n)

    def host_of(s):
        return lax.rem(i + s, n)

    def peer(dd, hh):
        return {"desc": lax.rem(d + dd, D), "half": lax.rem(h + hh, H)}

    def rows_of(d_at, h_at):
        return pl.ds(pl.multiple_of((d_at * H + h_at) * R, R), R)

    def chunk(c):
        return pl.ds(pl.multiple_of(c * CR, CR), CR)

    barrier = pltpu.get_barrier_semaphore()

    def greet(s, met):
        for active, at in ((visiting(s), host_of(s)), (hosting(s), guest_of(s))):
            @pl.when(active & (i < at))
            def _():
                pl.semaphore_signal(barrier, inc=1, device_id={"blk": at}, device_id_type=MESH)

            met = met + jnp.where(active & (at < i), 1, 0)
        return met

    met = lax.fori_loop(1, T + 1, greet, jnp.int32(0))
    for dd, hh in others:
        pl.semaphore_signal(barrier, inc=1, device_id=peer(dd, hh), device_id_type=MESH)
    pl.semaphore_wait(barrier, len(others) + met)

    def invite(s, carry):
        at = guest_of(s)

        @pl.when(hosting(s) & (at < i))
        def _():
            pl.semaphore_signal(go.at[s - 1], inc=1, device_id={"blk": at}, device_id_type=MESH)

        return carry

    lax.fori_loop(1, T + 1, invite, 0)

    def move(s, c):
        return pltpu.make_async_remote_copy(
            src_ref=x_ref.at[chunk(c)], dst_ref=buf.at[s - 1, chunk(c)],
            send_sem=z_send.at[s - 1, c], recv_sem=z_recv.at[s - 1, c],
            device_id={"blk": host_of(s)}, device_id_type=MESH,
        )

    mine_rows = rows_of(d, h)

    def query_copy(dd, hh):
        return pltpu.make_async_remote_copy(
            src_ref=x_ref, dst_ref=q.at[mine_rows],
            send_sem=q_send.at[dd * H + hh], recv_sem=q_recv.at[dd * H + hh],
            device_id=peer(dd, hh), device_id_type=MESH,
        )

    def query_relay(dd, hh):
        src_rows = rows_of(lax.rem(d + D - dd, D), h)
        return pltpu.make_async_remote_copy(
            src_ref=q.at[src_rows], dst_ref=q.at[src_rows],
            send_sem=q_send.at[dd * H + hh], recv_sem=q_recv.at[dd * H + hh],
            device_id=peer(0, hh), device_id_type=MESH,
        )

    load.wait()

    def move_down(s, carry):
        @pl.when(visiting(s) & (host_of(s) < i))
        def _():
            for c in range(CH):
                move(s, c).start()

        return carry

    lax.fori_loop(1, T + 1, move_down, 0)
    for dd in range(1, D):
        query_copy(dd, 0).start()
    for hh in range(1, H):
        query_copy(0, hh).start()
    q[mine_rows, :] = x_ref[...]

    def move_up(s, carry):
        @pl.when(visiting(s) & (host_of(s) > i))
        def _():
            pl.semaphore_wait(go.at[s - 1], 1)
            for c in range(CH):
                move(s, c).start()

        return carry

    lax.fori_loop(1, T + 1, move_up, 0)

    for dd in range(1, D):
        query_copy(dd, 0).wait_recv()
        for hh in range(1, H):
            query_relay(dd, hh).start()
    for dd in range(D):
        for hh in range(1, H):
            query_copy(dd, hh).wait_recv()

    def widen(t, carry):
        rows = pl.ds(pl.multiple_of(t * TQ, TQ), TQ)
        wide = q[rows, :].astype(jnp.float32)
        sn[rows, :] = jnp.broadcast_to(jnp.sum(wide * wide, axis=1, keepdims=True), (TQ, 128))
        return carry

    lax.fori_loop(0, Q // TQ, widen, 0)

    def result_copy(s, dd, hh):
        return pltpu.make_async_remote_copy(
            src_ref=mine.at[s - 1, lax.rem(d + dd, D)], dst_ref=inbox.at[s - 1, dd * H + hh],
            send_sem=p_send.at[s - 1, dd * H + hh], recv_sem=p_recv.at[s - 1, dd * H + hh],
            device_id=peer(dd, hh), device_id_type=MESH,
        )

    def return_copy(s, hh):
        return pltpu.make_async_remote_copy(
            src_ref=turned.at[s - 1], dst_ref=returned.at[s - 1, hh],
            send_sem=m_send.at[s - 1, hh], recv_sem=m_recv.at[s - 1, hh],
            device_id={"blk": guest_of(s), "half": lax.rem(h + hh, H)}, device_id_type=MESH,
        )

    def step_of(u):
        return jnp.where(2 * i < n, T - u, u + 1)

    inf = functools.partial(jnp.full, fill_value=jnp.inf, dtype=jnp.float32)

    def work(u, carry):
        s = step_of(u)

        @pl.when(hosting(s))
        def _():
            low[...] = inf(low.shape)
            sec[...] = inf(sec.shape)

            def part_of(c, carry):
                move(s, c).wait_recv()
                wide = buf[s - 1, chunk(c), :].astype(jnp.float32)
                norms = jnp.sum(wide * wide, axis=1, keepdims=True)
                scaled = (wide * -2.0).astype(jnp.bfloat16)
                for t in range(Q // TQ):
                    lanes = slice(t * TQ, (t + 1) * TQ)
                    lo, se = fold(nt_dot(scaled, q[lanes, :]) + norms, low[:, lanes], sec[:, lanes])
                    low[:, lanes] = lo
                    sec[:, lanes] = se
                lo, se = inf((8, CR)), inf((8, CR))
                for t in range(Q // TQ):
                    rows = slice(t * TQ, (t + 1) * TQ)
                    lo, se = fold(nt_dot(q[rows, :], scaled) + sn[rows, 0:1], lo, se)
                lo, se = across_rows(lo, se)
                turned[s - 1, c, 0:1, :] = lo
                turned[s - 1, c, 1:2, :] = se
                return carry

            lax.fori_loop(0, CH, part_of, 0)
            for t in range(D):
                lanes = slice(t * share, (t + 1) * share)
                lo, se = across_rows(low[:, lanes], sec[:, lanes])
                mine[s - 1, t, 0:1, :] = lo
                mine[s - 1, t, 1:2, :] = se
            for dd, hh in reversed(others):
                result_copy(s, dd, hh).start()
            for hh in range(H):
                return_copy(s, hh).start()

        return carry

    lax.fori_loop(0, T, work, 0)

    own = q[pl.ds(pl.multiple_of(d * share, share), share), :].astype(jnp.float32)
    square = own * own
    head = square.astype(jnp.bfloat16)
    tail = (square - head.astype(jnp.float32)).astype(jnp.bfloat16)
    ones = jnp.ones((8, q.shape[1]), jnp.bfloat16)
    norm_ref[...] = (nt_dot(ones, head) + nt_dot(ones, tail))[0:1]

    def sent(s, carry):
        @pl.when(visiting(s))
        def _():
            for c in range(CH):
                move(s, c).wait_send()

        return carry

    lax.fori_loop(1, T + 1, sent, 0)
    for dd in range(1, D):
        query_copy(dd, 0).wait_send()
        for hh in range(1, H):
            query_relay(dd, hh).wait_send()
    for hh in range(1, H):
        query_copy(0, hh).wait_send()

    def finish(u, carry):
        s = step_of(u)

        @pl.when(visiting(s))
        def _():
            for hh in range(H):
                return_copy(s, hh).wait_recv()
            for hh in range(H):
                for c in range(CH):
                    at = lax.rem(h + H - hh, H) * CH + c
                    lanes = pl.ds(pl.multiple_of(at * CR, CR), CR)
                    best_ref[n - s - 1, :, lanes] = returned[s - 1, hh, c, 0:1, :]
                    second_ref[n - s - 1, :, lanes] = returned[s - 1, hh, c, 1:2, :]

        @pl.when(hosting(s))
        def _():
            lo, se = mine[s - 1, d, 0:1, :], mine[s - 1, d, 1:2, :]
            for dd, hh in others:
                result_copy(s, dd, hh).wait_recv()
                at = dd * H + hh
                lo, se = combine(lo, se, inbox[s - 1, at, 0:1, :], inbox[s - 1, at, 1:2, :])
            best_ref[s - 1] = lo
            second_ref[s - 1] = se

        return carry

    lax.fori_loop(0, T, finish, 0)

    def sent_results(s, carry):
        @pl.when(hosting(s))
        def _():
            for dd, hh in others:
                result_copy(s, dd, hh).wait_send()
            for hh in range(H):
                return_copy(s, hh).wait_send()

        return carry

    lax.fori_loop(1, T + 1, sent_results, 0)


def solution(mesh):
    n, D, H = mesh.shape["blk"], mesh.shape["desc"], mesh.shape["half"]
    T = n // 2

    def per_device(descriptors):
        block = descriptors[0]
        R, depth = block.shape
        CH = 2 if R % 32 == 0 else 1
        CR = R // CH
        share = H * R
        out = pltpu.VMEM((n - 1, 1, share), jnp.float32)
        vmem = pl.BlockSpec(memory_space=pltpu.VMEM)
        lo, se, norms = pl.pallas_call(
            functools.partial(kernel, n, D, H, CH),
            out_shape=(out, out, pltpu.VMEM((1, share), jnp.float32)),
            in_specs=[pl.BlockSpec(memory_space=pltpu.HBM)],
            out_specs=(vmem, vmem, vmem),
            scratch_shapes=[
                pltpu.VMEM((R, depth), jnp.bfloat16),
                pltpu.VMEM((T, R, depth), jnp.bfloat16),
                pltpu.VMEM((D * share, depth), jnp.bfloat16),
                pltpu.VMEM((D * share, 128), jnp.float32),
                pltpu.VMEM((8, D * share), jnp.float32),
                pltpu.VMEM((8, D * share), jnp.float32),
                pltpu.VMEM((T, D, 2, share), jnp.float32),
                pltpu.VMEM((T, D * H, 2, share), jnp.float32),
                pltpu.VMEM((T, CH, 2, CR), jnp.float32),
                pltpu.VMEM((T, H, CH, 2, CR), jnp.float32),
                pltpu.SemaphoreType.DMA,
                pltpu.SemaphoreType.REGULAR((T,)),
                pltpu.SemaphoreType.DMA((T, CH)),
                pltpu.SemaphoreType.DMA((T, CH)),
                pltpu.SemaphoreType.DMA((D * H,)),
                pltpu.SemaphoreType.DMA((D * H,)),
                pltpu.SemaphoreType.DMA((T, D * H)),
                pltpu.SemaphoreType.DMA((T, D * H)),
                pltpu.SemaphoreType.DMA((T, H)),
                pltpu.SemaphoreType.DMA((T, H)),
            ],
            compiler_params=pltpu.CompilerParams(collective_id=0, has_side_effects=True),
        )(block)
        return norms + lo, norms + se

    in_specs = (P(("groups", "blk"), ("desc", "half"), None),)
    out_specs = (P(None, ("groups", "blk"), "desc"), P(None, ("groups", "blk"), "desc"))
    return jax.shard_map(
        per_device, mesh=mesh, in_specs=in_specs, out_specs=out_specs, check_vma=False
    )
```

```python
import functools

import jax
import jax.numpy as jnp
from jax import lax
from jax.experimental import pallas as pl
from jax.experimental.pallas import tpu as pltpu
from jax.sharding import PartitionSpec as P

MESH = pl.DeviceIdType.MESH


def combine(lo_a, se_a, lo_b, se_b):
    return (
        jnp.minimum(lo_a, lo_b),
        jnp.minimum(jnp.maximum(lo_a, lo_b), jnp.minimum(se_a, se_b)),
    )


def nt_dot(a, b):
    return lax.dot_general(a, b, (((1,), (1,)), ((), ())), preferred_element_type=jnp.float32)


def fold(part, norms, lo, se):
    wide = part.shape[1] // norms.shape[1]
    kept = [(lo, se), None]
    for r in range(part.shape[0] // 8):
        rows = slice(8 * r, 8 * r + 8)
        value = part[rows] + jnp.concatenate([norms[rows]] * wide, axis=1)
        if kept[r % 2] is None:
            kept[r % 2] = (value, jnp.full_like(value, jnp.inf))
        else:
            lo, se = kept[r % 2]
            kept[r % 2] = (jnp.minimum(lo, value), jnp.minimum(se, jnp.maximum(lo, value)))
    if kept[1] is None:
        return kept[0]
    return combine(*kept[0], *kept[1])


def across_rows(lo, se):
    for turn in (4, 2, 1):
        lo, se = combine(lo, se, pltpu.roll(lo, turn, 0), pltpu.roll(se, turn, 0))
    return lo[0:1], se[0:1]


def kernel(
    n, D, H, CH, x_hbm, best_ref, second_ref, norm_ref,
    x_ref, buf, q, q2, sn, low, sec, mine, inbox, turned, returned,
    x_sem, go, go_q, z_send, z_recv, q_send, q_recv, p_send, p_recv, m_send, m_recv,
):
    R = x_hbm.shape[0]
    load = pltpu.make_async_copy(x_hbm, x_ref, x_sem)
    load.start()
    CR = R // CH
    share = H * R
    Q = D * share
    TQ = min(256, share)
    T = n // 2
    i = lax.axis_index("blk")
    d = lax.axis_index("desc")
    h = lax.axis_index("half")
    others = [(dd, hh) for dd in range(D) for hh in range(H) if (dd, hh) != (0, 0)]

    if n % 2 == 0:
        hosts_tie = (i < T) == (lax.rem(lax.rem(i, T), 2) == 0)
    else:
        hosts_tie = i >= 0

    def hosting(s):
        return (2 * s != n) | hosts_tie

    def visiting(s):
        if n % 2 == 0:
            return (2 * s != n) | jnp.logical_not(hosts_tie)
        return 2 * s != n

    def guest_of(s):
        return lax.rem(i - s + n, n)

    def host_of(s):
        return lax.rem(i + s, n)

    def peer(dd, hh):
        return {"desc": lax.rem(d + dd, D), "half": lax.rem(h + hh, H)}

    def rows_of(d_at, h_at):
        return pl.ds(pl.multiple_of((d_at * H + h_at) * R, R), R)

    def chunk(c):
        return pl.ds(pl.multiple_of(c * CR, CR), CR)

    barrier = pltpu.get_barrier_semaphore()

    def greet(s, met):
        for active, at in ((visiting(s), host_of(s)), (hosting(s), guest_of(s))):
            @pl.when(active & (i < at))
            def _():
                pl.semaphore_signal(barrier, inc=1, device_id={"blk": at}, device_id_type=MESH)

            met = met + jnp.where(active & (at < i), 1, 0)
        return met

    met = lax.fori_loop(1, T + 1, greet, jnp.int32(0))
    for dd in range(1, D):
        @pl.when(d + dd < D)
        def _():
            pl.semaphore_signal(barrier, inc=1, device_id={"desc": d + dd}, device_id_type=MESH)
    for hh in range(1, H):
        pl.semaphore_signal(barrier, inc=1, device_id=peer(0, hh), device_id_type=MESH)
    pl.semaphore_wait(barrier, H - 1 + d + met)

    def invite(s, carry):
        at = guest_of(s)

        @pl.when(hosting(s) & (at < i))
        def _():
            pl.semaphore_signal(go.at[s - 1], inc=1, device_id={"blk": at}, device_id_type=MESH)

        return carry

    lax.fori_loop(1, T + 1, invite, 0)
    for dd in range(1, D):
        @pl.when(d >= dd)
        def _():
            pl.semaphore_signal(
                go_q.at[dd - 1], inc=1, device_id={"desc": d - dd}, device_id_type=MESH
            )

    def move(s, c):
        return pltpu.make_async_remote_copy(
            src_ref=x_ref.at[chunk(c)], dst_ref=buf.at[s - 1, chunk(c)],
            send_sem=z_send.at[s - 1, c], recv_sem=z_recv.at[s - 1, c],
            device_id={"blk": host_of(s)}, device_id_type=MESH,
        )

    mine_rows = rows_of(d, h)

    def query_copy(dd, hh):
        return pltpu.make_async_remote_copy(
            src_ref=x_ref, dst_ref=q.at[mine_rows],
            send_sem=q_send.at[dd * H + hh], recv_sem=q_recv.at[dd * H + hh],
            device_id=peer(dd, hh), device_id_type=MESH,
        )

    def query_relay(dd, hh):
        src_rows = rows_of(lax.rem(d + D - dd, D), h)
        return pltpu.make_async_remote_copy(
            src_ref=q.at[src_rows], dst_ref=q.at[src_rows],
            send_sem=q_send.at[dd * H + hh], recv_sem=q_recv.at[dd * H + hh],
            device_id=peer(0, hh), device_id_type=MESH,
        )

    load.wait()

    def move_down(s, carry):
        @pl.when(visiting(s) & (host_of(s) < i))
        def _():
            for c in range(CH):
                move(s, c).start()

        return carry

    lax.fori_loop(1, T + 1, move_down, 0)
    for hh in range(1, H):
        query_copy(0, hh).start()
    for dd in range(1, D):
        @pl.when(d + dd < D)
        def _():
            pl.semaphore_wait(go_q.at[dd - 1], 1)

        query_copy(dd, 0).start()

    def widen(rows):
        wide = q[rows, :].astype(jnp.float32)
        q2[rows, :] = (wide * -2.0).astype(jnp.bfloat16)
        sn[rows, :] = jnp.broadcast_to(jnp.sum(wide * wide, axis=1, keepdims=True), (R, 128))

    q[mine_rows, :] = x_ref[...]
    widen(mine_rows)

    def move_up(s, carry):
        @pl.when(visiting(s) & (host_of(s) > i))
        def _():
            pl.semaphore_wait(go.at[s - 1], 1)
            for c in range(CH):
                move(s, c).start()

        return carry

    lax.fori_loop(1, T + 1, move_up, 0)

    def from_peer(dd, hh):
        return rows_of(lax.rem(d + D - dd, D), lax.rem(h + H - hh, H))

    for hh in range(1, H):
        query_copy(0, hh).wait_recv()
        widen(from_peer(0, hh))
    for dd in range(1, D):
        query_copy(dd, 0).wait_recv()
        for hh in range(1, H):
            query_relay(dd, hh).start()
        widen(from_peer(dd, 0))
    for dd in range(1, D):
        for hh in range(1, H):
            query_copy(dd, hh).wait_recv()
            widen(from_peer(dd, hh))

    def result_copy(s, dd, hh):
        return pltpu.make_async_remote_copy(
            src_ref=mine.at[s - 1, lax.rem(d + dd, D)], dst_ref=inbox.at[s - 1, dd * H + hh],
            send_sem=p_send.at[s - 1, dd * H + hh], recv_sem=p_recv.at[s - 1, dd * H + hh],
            device_id=peer(dd, hh), device_id_type=MESH,
        )

    def return_copy(s, hh):
        return pltpu.make_async_remote_copy(
            src_ref=turned.at[s - 1], dst_ref=returned.at[s - 1, hh],
            send_sem=m_send.at[s - 1, hh], recv_sem=m_recv.at[s - 1, hh],
            device_id={"blk": guest_of(s), "half": lax.rem(h + hh, H)}, device_id_type=MESH,
        )

    inf = functools.partial(jnp.full, fill_value=jnp.inf, dtype=jnp.float32)

    def host_side(s, c):
        piece = buf[s - 1, chunk(c), :]
        wide = piece.astype(jnp.float32)
        norms = jnp.broadcast_to(jnp.sum(wide * wide, axis=1, keepdims=True), (CR, 128))
        for t in range(Q // TQ):
            lanes = slice(t * TQ, (t + 1) * TQ)
            lo, se = low[s - 1, :, lanes], sec[s - 1, :, lanes]
            lo, se = fold(nt_dot(piece, q2[lanes, :]), norms, lo, se)
            low[s - 1, :, lanes] = lo
            sec[s - 1, :, lanes] = se

    def host_send(s):
        for t in range(D):
            lanes = slice(t * share, (t + 1) * share)
            lo, se = across_rows(low[s - 1, :, lanes], sec[s - 1, :, lanes])
            mine[s - 1, t, 0:1, :] = lo
            mine[s - 1, t, 1:2, :] = se
        for dd, hh in reversed(others):
            result_copy(s, dd, hh).start()

    def guest_side(s, c):
        piece = buf[s - 1, chunk(c), :]
        lo, se = inf((8, CR)), inf((8, CR))
        for t in range(Q // TQ):
            rows = slice(t * TQ, (t + 1) * TQ)
            lo, se = fold(nt_dot(q2[rows, :], piece), sn[rows, :], lo, se)
        lo, se = across_rows(lo, se)
        turned[s - 1, c, 0:1, :] = lo
        turned[s - 1, c, 1:2, :] = se

    def guest_send(s):
        for hh in range(H):
            return_copy(s, hh).start()

    def meet(k, carry):
        s, c = k // CH + 1, lax.rem(k, CH)

        @pl.when(hosting(s))
        def _():
            move(s, c).wait_recv()

            @pl.when(c < CH - 1)
            def _():
                host_side(s, c)
                guest_side(s, c)

            @pl.when(c == CH - 1)
            def _():
                def side(turn, carry):
                    @pl.when((turn == 0) == (2 * i < n))
                    def _():
                        host_side(s, c)
                        host_send(s)

                    @pl.when((turn == 0) != (2 * i < n))
                    def _():
                        guest_side(s, c)
                        guest_send(s)

                    return carry

                lax.fori_loop(0, 2, side, 0)

        return carry

    low[...] = inf(low.shape)
    sec[...] = inf(sec.shape)
    lax.fori_loop(0, T * CH, meet, 0)

    own = q[pl.ds(pl.multiple_of(d * share, share), share), :].astype(jnp.float32)
    square = own * own
    head = square.astype(jnp.bfloat16)
    tail = (square - head.astype(jnp.float32)).astype(jnp.bfloat16)
    ones = jnp.ones((8, q.shape[1]), jnp.bfloat16)
    norm_ref[...] = (nt_dot(ones, head) + nt_dot(ones, tail))[0:1]

    def sent(s, carry):
        @pl.when(visiting(s))
        def _():
            for c in range(CH):
                move(s, c).wait_send()

        return carry

    lax.fori_loop(1, T + 1, sent, 0)
    for dd in range(1, D):
        query_copy(dd, 0).wait_send()
        for hh in range(1, H):
            query_relay(dd, hh).wait_send()
    for hh in range(1, H):
        query_copy(0, hh).wait_send()

    def finish(s, carry):
        @pl.when(visiting(s))
        def _():
            for hh in range(H):
                return_copy(s, hh).wait_recv()
            for hh in range(H):
                for c in range(CH):
                    at = lax.rem(h + H - hh, H) * CH + c
                    lanes = pl.ds(pl.multiple_of(at * CR, CR), CR)
                    best_ref[n - s - 1, :, lanes] = returned[s - 1, hh, c, 0:1, :]
                    second_ref[n - s - 1, :, lanes] = returned[s - 1, hh, c, 1:2, :]

        @pl.when(hosting(s))
        def _():
            lo, se = mine[s - 1, d, 0:1, :], mine[s - 1, d, 1:2, :]
            for dd, hh in others:
                result_copy(s, dd, hh).wait_recv()
                at = dd * H + hh
                lo, se = combine(lo, se, inbox[s - 1, at, 0:1, :], inbox[s - 1, at, 1:2, :])
            best_ref[s - 1] = lo
            second_ref[s - 1] = se

        return carry

    lax.fori_loop(1, T + 1, finish, 0)

    def sent_results(s, carry):
        @pl.when(hosting(s))
        def _():
            for dd, hh in others:
                result_copy(s, dd, hh).wait_send()
            for hh in range(H):
                return_copy(s, hh).wait_send()

        return carry

    lax.fori_loop(1, T + 1, sent_results, 0)


def solution(mesh):
    n, D, H = mesh.shape["blk"], mesh.shape["desc"], mesh.shape["half"]
    T = n // 2

    def per_device(descriptors):
        block = descriptors[0]
        R, depth = block.shape
        CH = 2 if R % 32 == 0 else 1
        CR = R // CH
        share = H * R
        out = pltpu.VMEM((n - 1, 1, share), jnp.float32)
        vmem = pl.BlockSpec(memory_space=pltpu.VMEM)
        lo, se, norms = pl.pallas_call(
            functools.partial(kernel, n, D, H, CH),
            out_shape=(out, out, pltpu.VMEM((1, share), jnp.float32)),
            in_specs=[pl.BlockSpec(memory_space=pltpu.HBM)],
            out_specs=(vmem, vmem, vmem),
            scratch_shapes=[
                pltpu.VMEM((R, depth), jnp.bfloat16),
                pltpu.VMEM((T, R, depth), jnp.bfloat16),
                pltpu.VMEM((D * share, depth), jnp.bfloat16),
                pltpu.VMEM((D * share, depth), jnp.bfloat16),
                pltpu.VMEM((D * share, 128), jnp.float32),
                pltpu.VMEM((T, 8, D * share), jnp.float32),
                pltpu.VMEM((T, 8, D * share), jnp.float32),
                pltpu.VMEM((T, D, 2, share), jnp.float32),
                pltpu.VMEM((T, D * H, 2, share), jnp.float32),
                pltpu.VMEM((T, CH, 2, CR), jnp.float32),
                pltpu.VMEM((T, H, CH, 2, CR), jnp.float32),
                pltpu.SemaphoreType.DMA,
                pltpu.SemaphoreType.REGULAR((T,)),
                pltpu.SemaphoreType.REGULAR((max(D - 1, 1),)),
                pltpu.SemaphoreType.DMA((T, CH)),
                pltpu.SemaphoreType.DMA((T, CH)),
                pltpu.SemaphoreType.DMA((D * H,)),
                pltpu.SemaphoreType.DMA((D * H,)),
                pltpu.SemaphoreType.DMA((T, D * H)),
                pltpu.SemaphoreType.DMA((T, D * H)),
                pltpu.SemaphoreType.DMA((T, H)),
                pltpu.SemaphoreType.DMA((T, H)),
            ],
            compiler_params=pltpu.CompilerParams(collective_id=0, has_side_effects=True),
        )(block)
        return norms + lo, norms + se

    in_specs = (P(("groups", "blk"), ("desc", "half"), None),)
    out_specs = (P(None, ("groups", "blk"), "desc"), P(None, ("groups", "blk"), "desc"))
    return jax.shard_map(
        per_device, mesh=mesh, in_specs=in_specs, out_specs=out_specs, check_vma=False
    )
```

```python
import functools

import jax
import jax.numpy as jnp
from jax import lax
from jax.experimental import pallas as pl
from jax.experimental.pallas import tpu as pltpu
from jax.sharding import PartitionSpec as P

MESH = pl.DeviceIdType.MESH


def combine(lo_a, se_a, lo_b, se_b):
    return (
        jnp.minimum(lo_a, lo_b),
        jnp.minimum(jnp.maximum(lo_a, lo_b), jnp.minimum(se_a, se_b)),
    )


def nt_dot(a, b):
    return lax.dot_general(a, b, (((1,), (1,)), ((), ())), preferred_element_type=jnp.float32)


def fold(part, norms, lo, se):
    wide = part.shape[1] // norms.shape[1]
    kept = [(lo, se), None]
    for r in range(part.shape[0] // 8):
        rows = slice(8 * r, 8 * r + 8)
        value = part[rows] + jnp.concatenate([norms[rows]] * wide, axis=1)
        if kept[r % 2] is None:
            kept[r % 2] = (value, jnp.full_like(value, jnp.inf))
        else:
            lo, se = kept[r % 2]
            kept[r % 2] = (jnp.minimum(lo, value), jnp.minimum(se, jnp.maximum(lo, value)))
    if kept[1] is None:
        return kept[0]
    return combine(*kept[0], *kept[1])


def across_rows(lo, se):
    for turn in (4, 2, 1):
        lo, se = combine(lo, se, pltpu.roll(lo, turn, 0), pltpu.roll(se, turn, 0))
    return lo[0:1], se[0:1]


def kernel(
    n, D, H, CH, x_hbm, best_ref, second_ref, norm_ref,
    x_ref, buf, q, q2, sn, low, sec, mine, inbox, turned, returned,
    x_sem, go, go_q, z_send, z_recv, y_send, y_recv, q_send, q_recv, p_send, p_recv, m_send, m_recv,
):
    R = x_hbm.shape[0]
    load = pltpu.make_async_copy(x_hbm, x_ref, x_sem)
    load.start()
    CR = R // CH
    share = H * R
    Q = D * share
    TQ = min(256, share)
    T = n // 2
    i = lax.axis_index("blk")
    d = lax.axis_index("desc")
    h = lax.axis_index("half")
    inf = functools.partial(jnp.full, fill_value=jnp.inf, dtype=jnp.float32)
    others = [(dd, hh) for dd in range(D) for hh in range(H) if (dd, hh) != (0, 0)]

    if n % 2 == 0:
        hosts_tie = (i < T) == (lax.rem(lax.rem(i, T), 2) == 0)
    else:
        hosts_tie = i >= 0

    def hosting(s):
        return (2 * s != n) | hosts_tie

    def visiting(s):
        if n % 2 == 0:
            return (2 * s != n) | jnp.logical_not(hosts_tie)
        return 2 * s != n

    def guest_of(s):
        return lax.rem(i - s + n, n)

    def host_of(s):
        return lax.rem(i + s, n)

    def peer(dd, hh):
        return {"desc": lax.rem(d + dd, D), "half": lax.rem(h + hh, H)}

    def rows_of(d_at, h_at):
        return pl.ds(pl.multiple_of((d_at * H + h_at) * R, R), R)

    def chunk(c):
        return pl.ds(pl.multiple_of(c * CR, CR), CR)

    barrier = pltpu.get_barrier_semaphore()

    def greet(s, met):
        for active, at in ((visiting(s), host_of(s)), (hosting(s), guest_of(s))):
            @pl.when(active & (i < at))
            def _():
                pl.semaphore_signal(barrier, inc=1, device_id={"blk": at}, device_id_type=MESH)

            met = met + jnp.where(active & (at < i), 1, 0)
        return met

    met = lax.fori_loop(1, T + 1, greet, jnp.int32(0))
    for dd in range(1, D):
        @pl.when(d + dd < D)
        def _():
            pl.semaphore_signal(barrier, inc=1, device_id={"desc": d + dd}, device_id_type=MESH)
    for hh in range(1, H):
        pl.semaphore_signal(barrier, inc=1, device_id=peer(0, hh), device_id_type=MESH)
    pl.semaphore_wait(barrier, H - 1 + d + met)

    def invite(s, carry):
        at = guest_of(s)

        @pl.when(hosting(s) & (at < i))
        def _():
            pl.semaphore_signal(go.at[s - 1], inc=1, device_id={"blk": at}, device_id_type=MESH)

        return carry

    lax.fori_loop(1, T + 1, invite, 0)
    for dd in range(1, D):
        @pl.when(d >= dd)
        def _():
            pl.semaphore_signal(
                go_q.at[dd - 1], inc=1, device_id={"desc": d - dd}, device_id_type=MESH
            )

    detour = n % 2 == 0 and D > 1 and H > 1 and CH == 2
    gains = (i == 0) & (d == 0) & (h == H - 1) if detour else i < 0

    def keeps(s, c, guest):
        if not detour:
            return i >= 0
        elsewhere = (d != 1) | (h != 0) | (i != (T if guest else 0))
        return (s != T) | (c != CH - 1) | elsewhere

    def move(s, c):
        return pltpu.make_async_remote_copy(
            src_ref=x_ref.at[chunk(c)], dst_ref=buf.at[s - 1, chunk(c)],
            send_sem=z_send.at[s - 1, c], recv_sem=z_recv.at[s - 1, c],
            device_id={"blk": host_of(s)}, device_id_type=MESH,
        )

    mine_rows = rows_of(d, h)

    def part_of(d_at, h_at, c):
        return pl.ds(pl.multiple_of((d_at * H + h_at) * R + c * CR, CR), CR)

    def query_copy(dd, hh, c):
        return pltpu.make_async_remote_copy(
            src_ref=x_ref.at[chunk(c)], dst_ref=q.at[part_of(d, h, c)],
            send_sem=q_send.at[dd * H + hh, c], recv_sem=q_recv.at[dd * H + hh, c],
            device_id=peer(dd, hh), device_id_type=MESH,
        )

    def query_relay(dd, hh, c):
        rows = part_of(lax.rem(d + D - dd, D), h, c)
        return pltpu.make_async_remote_copy(
            src_ref=q.at[rows], dst_ref=q.at[rows],
            send_sem=q_send.at[dd * H + hh, c], recv_sem=q_recv.at[dd * H + hh, c],
            device_id=peer(0, hh), device_id_type=MESH,
        )

    def detour_copy():
        return pltpu.make_async_remote_copy(
            src_ref=q.at[part_of(1, 0, CH - 1)], dst_ref=buf.at[T, chunk(0)],
            send_sem=y_send, recv_sem=y_recv,
            device_id={"blk": i - T, "half": H - 1}, device_id_type=MESH,
        )

    load.wait()

    def move_down(s, carry):
        for c in range(CH):
            @pl.when(visiting(s) & (host_of(s) < i) & keeps(s, c, True))
            def _():
                move(s, c).start()

        return carry

    lax.fori_loop(1, T + 1, move_down, 0)
    for hh in range(1, H):
        for c in range(CH):
            query_copy(0, hh, c).start()
    for dd in range(1, D):
        @pl.when(d + dd < D)
        def _():
            pl.semaphore_wait(go_q.at[dd - 1], 1)

        for c in reversed(range(CH)):
            query_copy(dd, 0, c).start()

    def widen(rows):
        wide = q[rows, :].astype(jnp.float32)
        q2[rows, :] = (wide * -2.0).astype(jnp.bfloat16)
        sn[rows, :] = jnp.broadcast_to(jnp.sum(wide * wide, axis=1, keepdims=True), (R, 128))

    q[mine_rows, :] = x_ref[...]
    widen(mine_rows)

    def move_up(s, carry):
        @pl.when(visiting(s) & (host_of(s) > i))
        def _():
            pl.semaphore_wait(go.at[s - 1], 1)
            for c in range(CH):
                move(s, c).start()

        return carry

    lax.fori_loop(1, T + 1, move_up, 0)

    def from_peer(dd, hh):
        return rows_of(lax.rem(d + D - dd, D), lax.rem(h + H - hh, H))

    for hh in range(1, H):
        for c in range(CH):
            query_copy(0, hh, c).wait_recv()
        widen(from_peer(0, hh))
    own = q[pl.ds(pl.multiple_of(d * share, share), share), :].astype(jnp.float32)
    square = own * own
    head = square.astype(jnp.bfloat16)
    tail = (square - head.astype(jnp.float32)).astype(jnp.bfloat16)
    ones = jnp.ones((8, q.shape[1]), jnp.bfloat16)
    norm_ref[...] = (nt_dot(ones, head) + nt_dot(ones, tail))[0:1]
    low[...] = inf(low.shape)
    sec[...] = inf(sec.shape)
    for dd in range(1, D):
        for c in reversed(range(CH)):
            query_copy(dd, 0, c).wait_recv()
            if detour and c == CH - 1 and dd == D - 1:
                @pl.when((i == T) & (d == 0) & (h == 0))
                def _():
                    detour_copy().start()
            for hh in range(1, H):
                query_relay(dd, hh, c).start()
        widen(from_peer(dd, 0))
    for dd in range(1, D):
        for hh in range(1, H):
            for c in range(CH):
                query_copy(dd, hh, c).wait_recv()
            widen(from_peer(dd, hh))

    def result_copy(s, dd, hh):
        return pltpu.make_async_remote_copy(
            src_ref=mine.at[s - 1, lax.rem(d + dd, D)], dst_ref=inbox.at[s - 1, dd * H + hh],
            send_sem=p_send.at[s - 1, dd * H + hh], recv_sem=p_recv.at[s - 1, dd * H + hh],
            device_id=peer(dd, hh), device_id_type=MESH,
        )

    def return_copy(s, hh, c):
        return pltpu.make_async_remote_copy(
            src_ref=turned.at[s - 1, c], dst_ref=returned.at[s - 1, hh, c],
            send_sem=m_send.at[s - 1, hh, c], recv_sem=m_recv.at[s - 1, hh, c],
            device_id={"blk": guest_of(s), "half": lax.rem(h + hh, H)}, device_id_type=MESH,
        )

    def detour_return(hh):
        return pltpu.make_async_remote_copy(
            src_ref=turned.at[T, 0], dst_ref=returned.at[T - 1, hh, CH - 1],
            send_sem=m_send.at[T, hh, 0], recv_sem=m_recv.at[T - 1, hh, CH - 1],
            device_id={"blk": i + T, "desc": 1, "half": hh},
            device_id_type=MESH,
        )

    def host_side(s, at, c):
        piece = buf[at, chunk(c), :]
        wide = piece.astype(jnp.float32)
        norms = jnp.broadcast_to(jnp.sum(wide * wide, axis=1, keepdims=True), (CR, 128))
        for t in range(Q // TQ):
            lanes = slice(t * TQ, (t + 1) * TQ)
            lo, se = low[s - 1, :, lanes], sec[s - 1, :, lanes]
            lo, se = fold(nt_dot(piece, q2[lanes, :]), norms, lo, se)
            low[s - 1, :, lanes] = lo
            sec[s - 1, :, lanes] = se

    def host_send(s):
        for t in range(D):
            lanes = slice(t * share, (t + 1) * share)
            lo, se = across_rows(low[s - 1, :, lanes], sec[s - 1, :, lanes])
            mine[s - 1, t, 0:1, :] = lo
            mine[s - 1, t, 1:2, :] = se
        for dd, hh in reversed(others):
            result_copy(s, dd, hh).start()

    def guest_side(at, rows, width):
        piece = buf[at, rows, :]
        lo, se = inf((8, width)), inf((8, width))
        for t in range(Q // TQ):
            rows = slice(t * TQ, (t + 1) * TQ)
            lo, se = fold(nt_dot(q2[rows, :], piece), sn[rows, :], lo, se)
        return across_rows(lo, se)

    def guest_chunk(s, at, c):
        lo, se = guest_side(at, chunk(c), CR)
        turned[at, c, 0:1, :] = lo
        turned[at, c, 1:2, :] = se

        @pl.when(at < T)
        def _():
            for hh in range(H):
                return_copy(s, hh, c).start()

        if detour:
            @pl.when(at == T)
            def _():
                for hh in range(H):
                    detour_return(hh).start()

    def guest_whole(s):
        lo, se = guest_side(s - 1, slice(0, R), R)
        for c in range(CH):
            lanes = slice(c * CR, (c + 1) * CR)
            turned[s - 1, c, 0:1, :] = lo[:, lanes]
            turned[s - 1, c, 1:2, :] = se[:, lanes]
            for hh in range(H):
                return_copy(s, hh, c).start()

    def turn_of(k):
        rest = (T - 1) * CH
        upper = (2 * i >= n) & (k > 0)
        far = upper & (k <= rest)
        s = jnp.where(upper, jnp.where(far, 1 + (k + CH - 1) // CH, 1), k // CH + 1)
        c = jnp.where(upper, jnp.where(far, lax.rem(k + CH - 1, CH), k - rest), lax.rem(k, CH))
        return s, c

    items = T * CH + (1 if detour else 0)

    def meet(k, carry):
        s, c = turn_of(k)
        at = s - 1
        comes = hosting(s) & keeps(s, c, False)
        closes = (c == CH - 1) & jnp.logical_not(gains & (s == T))
        lost, extra = i < 0, i < 0
        if detour:
            extra = k == T * CH
            s, c, at = jnp.where(extra, T, s), jnp.where(extra, 0, c), jnp.where(extra, T, at)
            comes = jnp.where(extra, gains, comes)
            lost = jnp.logical_not(keeps(s, CH - 1, False))
            closes = extra | closes | (lost & (c == CH - 2))

        @pl.when(comes & (at < T))
        def _():
            move(s, c).wait_recv()

        if detour:
            @pl.when(comes & (at == T))
            def _():
                detour_copy().wait_recv()

        lower = 2 * i < n
        both = comes & jnp.logical_not(closes) & jnp.logical_not(lower)

        @pl.when(both)
        def _():
            host_side(s, at, c)
            guest_chunk(s, at, c)

        def side(turn, carry):
            host_turn = (turn == 0) == (lower | (s != T))

            @pl.when(host_turn & comes)
            def _():
                host_side(s, at, c)

                @pl.when(closes)
                def _():
                    host_send(s)

            guest_turn = jnp.logical_not(host_turn) & comes & closes

            @pl.when(guest_turn & lower & (extra | jnp.logical_not(lost)))
            def _():
                guest_whole(s)

            @pl.when(guest_turn & (jnp.logical_not(lower) | lost | extra))
            def _():
                guest_chunk(s, at, c)

            return carry

        lax.fori_loop(0, jnp.where(both, 0, 2), side, 0)
        return carry

    lax.fori_loop(0, items, meet, 0)

    def sent(s, carry):
        for c in range(CH):
            @pl.when(visiting(s) & keeps(s, c, True))
            def _():
                move(s, c).wait_send()

        return carry

    lax.fori_loop(1, T + 1, sent, 0)
    if detour:
        @pl.when((i == T) & (d == 0) & (h == 0))
        def _():
            detour_copy().wait_send()
    for c in range(CH):
        for dd in range(1, D):
            query_copy(dd, 0, c).wait_send()
            for hh in range(1, H):
                query_relay(dd, hh, c).wait_send()
        for hh in range(1, H):
            query_copy(0, hh, c).wait_send()

    def finish(s, carry):
        @pl.when(visiting(s))
        def _():
            for hh in range(H):
                for c in range(CH):
                    return_copy(s, hh, c).wait_recv()
            for hh in range(H):
                for c in range(CH):
                    at = lax.rem(h + H - hh, H) * CH + c
                    lanes = pl.ds(pl.multiple_of(at * CR, CR), CR)
                    best_ref[n - s - 1, :, lanes] = returned[s - 1, hh, c, 0:1, :]
                    second_ref[n - s - 1, :, lanes] = returned[s - 1, hh, c, 1:2, :]

        @pl.when(hosting(s))
        def _():
            lo, se = mine[s - 1, d, 0:1, :], mine[s - 1, d, 1:2, :]
            for dd, hh in others:
                result_copy(s, dd, hh).wait_recv()
                at = dd * H + hh
                lo, se = combine(lo, se, inbox[s - 1, at, 0:1, :], inbox[s - 1, at, 1:2, :])
            best_ref[s - 1] = lo
            second_ref[s - 1] = se

        return carry

    lax.fori_loop(1, T + 1, finish, 0)

    def sent_results(s, carry):
        @pl.when(hosting(s))
        def _():
            for dd, hh in others:
                result_copy(s, dd, hh).wait_send()

        for c in range(CH):
            @pl.when(hosting(s) & keeps(s, c, False))
            def _():
                for hh in range(H):
                    return_copy(s, hh, c).wait_send()

        return carry

    lax.fori_loop(1, T + 1, sent_results, 0)
    if detour:
        @pl.when(gains)
        def _():
            for hh in range(H):
                detour_return(hh).wait_send()


def solution(mesh):
    n, D, H = mesh.shape["blk"], mesh.shape["desc"], mesh.shape["half"]
    T = n // 2

    def per_device(descriptors):
        block = descriptors[0]
        R, depth = block.shape
        CH = 2 if R % 32 == 0 else 1
        CR = R // CH
        share = H * R
        out = pltpu.VMEM((n - 1, 1, share), jnp.float32)
        vmem = pl.BlockSpec(memory_space=pltpu.VMEM)
        lo, se, norms = pl.pallas_call(
            functools.partial(kernel, n, D, H, CH),
            out_shape=(out, out, pltpu.VMEM((1, share), jnp.float32)),
            in_specs=[pl.BlockSpec(memory_space=pltpu.HBM)],
            out_specs=(vmem, vmem, vmem),
            scratch_shapes=[
                pltpu.VMEM((R, depth), jnp.bfloat16),
                pltpu.VMEM((T + 1, R, depth), jnp.bfloat16),
                pltpu.VMEM((D * share, depth), jnp.bfloat16),
                pltpu.VMEM((D * share, depth), jnp.bfloat16),
                pltpu.VMEM((D * share, 128), jnp.float32),
                pltpu.VMEM((T, 8, D * share), jnp.float32),
                pltpu.VMEM((T, 8, D * share), jnp.float32),
                pltpu.VMEM((T, D, 2, share), jnp.float32),
                pltpu.VMEM((T, D * H, 2, share), jnp.float32),
                pltpu.VMEM((T + 1, CH, 2, CR), jnp.float32),
                pltpu.VMEM((T, H, CH, 2, CR), jnp.float32),
                pltpu.SemaphoreType.DMA,
                pltpu.SemaphoreType.REGULAR((T,)),
                pltpu.SemaphoreType.REGULAR((max(D - 1, 1),)),
                pltpu.SemaphoreType.DMA((T, CH)),
                pltpu.SemaphoreType.DMA((T, CH)),
                pltpu.SemaphoreType.DMA,
                pltpu.SemaphoreType.DMA,
                pltpu.SemaphoreType.DMA((D * H, CH)),
                pltpu.SemaphoreType.DMA((D * H, CH)),
                pltpu.SemaphoreType.DMA((T, D * H)),
                pltpu.SemaphoreType.DMA((T, D * H)),
                pltpu.SemaphoreType.DMA((T + 1, H, CH)),
                pltpu.SemaphoreType.DMA((T, H, CH)),
            ],
            compiler_params=pltpu.CompilerParams(collective_id=0, has_side_effects=True),
        )(block)
        return norms + lo, norms + se

    in_specs = (P(("groups", "blk"), ("desc", "half"), None),)
    out_specs = (P(None, ("groups", "blk"), "desc"), P(None, ("groups", "blk"), "desc"))
    return jax.shard_map(
        per_device, mesh=mesh, in_specs=in_specs, out_specs=out_specs, check_vma=False
    )
```

```python
import functools

import jax
import jax.numpy as jnp
from jax import lax
from jax.experimental import pallas as pl
from jax.experimental.pallas import tpu as pltpu
from jax.sharding import PartitionSpec as P

MESH = pl.DeviceIdType.MESH


def combine(lo_a, se_a, lo_b, se_b):
    return (
        jnp.minimum(lo_a, lo_b),
        jnp.minimum(jnp.maximum(lo_a, lo_b), jnp.minimum(se_a, se_b)),
    )


def nt_dot(a, b):
    return lax.dot_general(a, b, (((1,), (1,)), ((), ())), preferred_element_type=jnp.float32)


def fold(part, norms, lo, se):
    wide = part.shape[1] // norms.shape[1]
    kept = [(lo, se), None]
    for r in range(part.shape[0] // 8):
        rows = slice(8 * r, 8 * r + 8)
        value = part[rows] + jnp.concatenate([norms[rows]] * wide, axis=1)
        if kept[r % 2] is None:
            kept[r % 2] = (value, jnp.full_like(value, jnp.inf))
        else:
            lo, se = kept[r % 2]
            kept[r % 2] = (jnp.minimum(lo, value), jnp.minimum(se, jnp.maximum(lo, value)))
    if kept[1] is None:
        return kept[0]
    return combine(*kept[0], *kept[1])


def across_rows(lo, se):
    for turn in (4, 2, 1):
        lo, se = combine(lo, se, pltpu.roll(lo, turn, 0), pltpu.roll(se, turn, 0))
    return lo[0:1], se[0:1]


def kernel(
    n, D, H, CH, x_hbm, best_ref, second_ref, norm_ref,
    x_ref, buf, q, q2, sn, low, sec, mine, inbox, turned, returned,
    x_sem, go, go_q, z_send, z_recv, y_send, y_recv, q_send, q_recv, p_send, p_recv, m_send, m_recv,
):
    R = x_hbm.shape[0]
    load = pltpu.make_async_copy(x_hbm, x_ref, x_sem)
    load.start()
    CR = R // CH
    share = H * R
    Q = D * share
    TQ = min(256, share)
    T = n // 2
    i = lax.axis_index("blk")
    d = lax.axis_index("desc")
    h = lax.axis_index("half")
    inf = functools.partial(jnp.full, fill_value=jnp.inf, dtype=jnp.float32)
    others = [(dd, hh) for dd in range(D) for hh in range(H) if (dd, hh) != (0, 0)]

    if n % 2 == 0:
        hosts_tie = (i < T) == (lax.rem(lax.rem(i, T), 2) == 0)
    else:
        hosts_tie = i >= 0

    def hosting(s):
        return (2 * s != n) | hosts_tie

    def visiting(s):
        if n % 2 == 0:
            return (2 * s != n) | jnp.logical_not(hosts_tie)
        return 2 * s != n

    def guest_of(s):
        return lax.rem(i - s + n, n)

    def host_of(s):
        return lax.rem(i + s, n)

    def peer(dd, hh):
        return {"desc": lax.rem(d + dd, D), "half": lax.rem(h + hh, H)}

    def rows_of(d_at, h_at):
        return pl.ds(pl.multiple_of((d_at * H + h_at) * R, R), R)

    def chunk(c):
        return pl.ds(pl.multiple_of(c * CR, CR), CR)

    barrier = pltpu.get_barrier_semaphore()

    def greet(s, met):
        for active, at in ((visiting(s), host_of(s)), (hosting(s), guest_of(s))):
            @pl.when(active & (i < at))
            def _():
                pl.semaphore_signal(barrier, inc=1, device_id={"blk": at}, device_id_type=MESH)

            met = met + jnp.where(active & (at < i), 1, 0)
        return met

    met = lax.fori_loop(1, T + 1, greet, jnp.int32(0))
    for dd in range(1, D):
        @pl.when(d + dd < D)
        def _():
            pl.semaphore_signal(barrier, inc=1, device_id={"desc": d + dd}, device_id_type=MESH)
    for hh in range(1, H):
        pl.semaphore_signal(barrier, inc=1, device_id=peer(0, hh), device_id_type=MESH)
    pl.semaphore_wait(barrier, H - 1 + d + met)

    def invite(s, carry):
        at = guest_of(s)

        @pl.when(hosting(s) & (at < i))
        def _():
            pl.semaphore_signal(go.at[s - 1], inc=1, device_id={"blk": at}, device_id_type=MESH)

        return carry

    lax.fori_loop(1, T + 1, invite, 0)
    for dd in range(1, D):
        @pl.when(d >= dd)
        def _():
            pl.semaphore_signal(
                go_q.at[dd - 1], inc=1, device_id={"desc": d - dd}, device_id_type=MESH
            )

    detour = n % 2 == 0 and D > 1 and H > 1 and CH == 2
    gains = (i == 0) & (d == 0) & (h == H - 1) if detour else i < 0

    def keeps(s, c, guest):
        if not detour:
            return i >= 0
        elsewhere = (d != 1) | (h != 0) | (i != (T if guest else 0))
        return (s != T) | (c != CH - 1) | elsewhere

    def move(s, c):
        return pltpu.make_async_remote_copy(
            src_ref=x_ref.at[chunk(c)], dst_ref=buf.at[s - 1, chunk(c)],
            send_sem=z_send.at[s - 1, c], recv_sem=z_recv.at[s - 1, c],
            device_id={"blk": host_of(s)}, device_id_type=MESH,
        )

    mine_rows = rows_of(d, h)

    def part_of(d_at, h_at, c):
        return pl.ds(pl.multiple_of((d_at * H + h_at) * R + c * CR, CR), CR)

    def query_copy(dd, hh, c):
        return pltpu.make_async_remote_copy(
            src_ref=x_ref.at[chunk(c)], dst_ref=q.at[part_of(d, h, c)],
            send_sem=q_send.at[dd * H + hh, c], recv_sem=q_recv.at[dd * H + hh, c],
            device_id=peer(dd, hh), device_id_type=MESH,
        )

    def query_relay(dd, hh, c):
        rows = part_of(lax.rem(d + D - dd, D), h, c)
        return pltpu.make_async_remote_copy(
            src_ref=q.at[rows], dst_ref=q.at[rows],
            send_sem=q_send.at[dd * H + hh, c], recv_sem=q_recv.at[dd * H + hh, c],
            device_id=peer(0, hh), device_id_type=MESH,
        )

    def detour_copy():
        return pltpu.make_async_remote_copy(
            src_ref=q.at[part_of(1, 0, CH - 1)], dst_ref=buf.at[T, chunk(0)],
            send_sem=y_send, recv_sem=y_recv,
            device_id={"blk": i - T, "half": H - 1}, device_id_type=MESH,
        )

    load.wait()

    def move_down(s, carry):
        for c in range(CH):
            @pl.when(visiting(s) & (host_of(s) < i) & keeps(s, c, True))
            def _():
                move(s, c).start()

        return carry

    lax.fori_loop(1, T + 1, move_down, 0)
    for hh in range(1, H):
        for c in range(CH):
            query_copy(0, hh, c).start()
    for dd in range(1, D):
        @pl.when(d + dd < D)
        def _():
            pl.semaphore_wait(go_q.at[dd - 1], 1)

        for c in reversed(range(CH)):
            query_copy(dd, 0, c).start()

    def widen(rows):
        wide = q[rows, :].astype(jnp.float32)
        q2[rows, :] = (wide * -2.0).astype(jnp.bfloat16)
        sn[rows, :] = jnp.broadcast_to(jnp.sum(wide * wide, axis=1, keepdims=True), (R, 128))

    q[mine_rows, :] = x_ref[...]
    widen(mine_rows)

    def move_up(s, carry):
        @pl.when(visiting(s) & (host_of(s) > i))
        def _():
            pl.semaphore_wait(go.at[s - 1], 1)
            for c in range(CH):
                move(s, c).start()

        return carry

    lax.fori_loop(1, T + 1, move_up, 0)

    def from_peer(dd, hh):
        return rows_of(lax.rem(d + D - dd, D), lax.rem(h + H - hh, H))

    for hh in range(1, H):
        for c in range(CH):
            query_copy(0, hh, c).wait_recv()
        widen(from_peer(0, hh))
    own = q[pl.ds(pl.multiple_of(d * share, share), share), :].astype(jnp.float32)
    square = own * own
    head = square.astype(jnp.bfloat16)
    tail = (square - head.astype(jnp.float32)).astype(jnp.bfloat16)
    ones = jnp.ones((8, q.shape[1]), jnp.bfloat16)
    norm_ref[...] = (nt_dot(ones, head) + nt_dot(ones, tail))[0:1]
    low[...] = inf(low.shape)
    sec[...] = inf(sec.shape)
    for dd in range(1, D):
        for c in reversed(range(CH)):
            query_copy(dd, 0, c).wait_recv()
            if detour and c == CH - 1 and dd == D - 1:
                @pl.when((i == T) & (d == 0) & (h == 0))
                def _():
                    detour_copy().start()
            for hh in range(1, H):
                query_relay(dd, hh, c).start()
        widen(from_peer(dd, 0))
    for dd in range(1, D):
        for hh in range(1, H):
            for c in range(CH):
                query_copy(dd, hh, c).wait_recv()
            widen(from_peer(dd, hh))

    def result_copy(s, dd, hh):
        return pltpu.make_async_remote_copy(
            src_ref=mine.at[s - 1, lax.rem(d + dd, D)], dst_ref=inbox.at[s - 1, dd * H + hh],
            send_sem=p_send.at[s - 1, dd * H + hh], recv_sem=p_recv.at[s - 1, dd * H + hh],
            device_id=peer(dd, hh), device_id_type=MESH,
        )

    def return_copy(s, hh, c):
        return pltpu.make_async_remote_copy(
            src_ref=turned.at[s - 1, c], dst_ref=returned.at[s - 1, hh, c],
            send_sem=m_send.at[s - 1, hh, c], recv_sem=m_recv.at[s - 1, hh, c],
            device_id={"blk": guest_of(s), "half": lax.rem(h + hh, H)}, device_id_type=MESH,
        )

    def detour_return(hh):
        return pltpu.make_async_remote_copy(
            src_ref=turned.at[T, 0], dst_ref=returned.at[T - 1, hh, CH - 1],
            send_sem=m_send.at[T, hh, 0], recv_sem=m_recv.at[T - 1, hh, CH - 1],
            device_id={"blk": i + T, "desc": 1, "half": hh},
            device_id_type=MESH,
        )

    def host_side(s, at, c):
        piece = buf[at, chunk(c), :]
        wide = piece.astype(jnp.float32)
        norms = jnp.broadcast_to(jnp.sum(wide * wide, axis=1, keepdims=True), (CR, 128))
        for t in range(Q // TQ):
            lanes = slice(t * TQ, (t + 1) * TQ)
            lo, se = low[s - 1, :, lanes], sec[s - 1, :, lanes]
            lo, se = fold(nt_dot(piece, q2[lanes, :]), norms, lo, se)
            low[s - 1, :, lanes] = lo
            sec[s - 1, :, lanes] = se

    def host_send(s):
        for t in range(D):
            lanes = slice(t * share, (t + 1) * share)
            lo, se = across_rows(low[s - 1, :, lanes], sec[s - 1, :, lanes])
            mine[s - 1, t, 0:1, :] = lo
            mine[s - 1, t, 1:2, :] = se
        for dd, hh in reversed(others):
            result_copy(s, dd, hh).start()

    def guest_side(at, rows, width):
        piece = buf[at, rows, :]
        lo, se = inf((8, width)), inf((8, width))
        for t in range(Q // TQ):
            rows = slice(t * TQ, (t + 1) * TQ)
            lo, se = fold(nt_dot(q2[rows, :], piece), sn[rows, :], lo, se)
        return across_rows(lo, se)

    def guest_chunk(s, at, c):
        lo, se = guest_side(at, chunk(c), CR)
        turned[at, c, 0:1, :] = lo
        turned[at, c, 1:2, :] = se

        @pl.when(at < T)
        def _():
            for hh in range(H):
                return_copy(s, hh, c).start()

        if detour:
            @pl.when(at == T)
            def _():
                for hh in range(H):
                    detour_return(hh).start()

    def guest_whole(s):
        lo, se = guest_side(s - 1, slice(0, R), R)
        for c in range(CH):
            lanes = slice(c * CR, (c + 1) * CR)
            turned[s - 1, c, 0:1, :] = lo[:, lanes]
            turned[s - 1, c, 1:2, :] = se[:, lanes]
            for hh in range(H):
                return_copy(s, hh, c).start()

    def turn_of(k):
        rest = (T - 1) * CH
        upper = (2 * i >= n) & (k > 0)
        far = upper & (k <= rest)
        s = jnp.where(upper, jnp.where(far, 1 + (k + CH - 1) // CH, 1), k // CH + 1)
        c = jnp.where(upper, jnp.where(far, lax.rem(k + CH - 1, CH), k - rest), lax.rem(k, CH))
        return s, c

    items = T * CH + (1 if detour else 0)

    def meet(k, carry):
        s, c = turn_of(k)
        at = s - 1
        comes = hosting(s) & keeps(s, c, False)
        closes = (c == CH - 1) & jnp.logical_not(gains & (s == T))
        lost, extra = i < 0, i < 0
        if detour:
            extra = k == T * CH
            s, c, at = jnp.where(extra, T, s), jnp.where(extra, 0, c), jnp.where(extra, T, at)
            comes = jnp.where(extra, gains, comes)
            lost = jnp.logical_not(keeps(s, CH - 1, False))
            closes = extra | closes | (lost & (c == CH - 2))

        @pl.when(comes & (at < T))
        def _():
            move(s, c).wait_recv()

        if detour:
            @pl.when(comes & (at == T))
            def _():
                detour_copy().wait_recv()

        lower = 2 * i < n

        @pl.when(comes & jnp.logical_not(lower))
        def _():
            host_side(s, at, c)
            guest_chunk(s, at, c)

            @pl.when(closes)
            def _():
                host_send(s)

        @pl.when(comes & lower)
        def _():
            host_side(s, at, c)

            @pl.when(closes)
            def _():
                host_send(s)

            whole = closes & (extra | jnp.logical_not(lost))

            @pl.when(whole & ((d == 0) | (s == T)))
            def _():
                guest_whole(s)

            @pl.when(extra | (closes & lost))
            def _():
                guest_chunk(s, at, c)

        return carry

    lax.fori_loop(0, items, meet, 0)

    def put_off(s, carry):
        @pl.when((2 * i < n) & (d > 0) & hosting(s))
        def _():
            guest_whole(s)

        return carry

    lax.fori_loop(1, T, put_off, 0)

    def sent(s, carry):
        for c in range(CH):
            @pl.when(visiting(s) & keeps(s, c, True))
            def _():
                move(s, c).wait_send()

        return carry

    lax.fori_loop(1, T + 1, sent, 0)
    if detour:
        @pl.when((i == T) & (d == 0) & (h == 0))
        def _():
            detour_copy().wait_send()
    for c in range(CH):
        for dd in range(1, D):
            query_copy(dd, 0, c).wait_send()
            for hh in range(1, H):
                query_relay(dd, hh, c).wait_send()
        for hh in range(1, H):
            query_copy(0, hh, c).wait_send()

    def finish(s, carry):
        @pl.when(visiting(s))
        def _():
            for hh in range(H):
                for c in range(CH):
                    return_copy(s, hh, c).wait_recv()
            for hh in range(H):
                for c in range(CH):
                    at = lax.rem(h + H - hh, H) * CH + c
                    lanes = pl.ds(pl.multiple_of(at * CR, CR), CR)
                    best_ref[n - s - 1, :, lanes] = returned[s - 1, hh, c, 0:1, :]
                    second_ref[n - s - 1, :, lanes] = returned[s - 1, hh, c, 1:2, :]

        @pl.when(hosting(s))
        def _():
            lo, se = mine[s - 1, d, 0:1, :], mine[s - 1, d, 1:2, :]
            for dd, hh in others:
                result_copy(s, dd, hh).wait_recv()
                at = dd * H + hh
                lo, se = combine(lo, se, inbox[s - 1, at, 0:1, :], inbox[s - 1, at, 1:2, :])
            best_ref[s - 1] = lo
            second_ref[s - 1] = se

        return carry

    lax.fori_loop(1, T + 1, finish, 0)

    def sent_results(s, carry):
        @pl.when(hosting(s))
        def _():
            for dd, hh in others:
                result_copy(s, dd, hh).wait_send()

        for c in range(CH):
            @pl.when(hosting(s) & keeps(s, c, False))
            def _():
                for hh in range(H):
                    return_copy(s, hh, c).wait_send()

        return carry

    lax.fori_loop(1, T + 1, sent_results, 0)
    if detour:
        @pl.when(gains)
        def _():
            for hh in range(H):
                detour_return(hh).wait_send()


def solution(mesh):
    n, D, H = mesh.shape["blk"], mesh.shape["desc"], mesh.shape["half"]
    T = n // 2

    def per_device(descriptors):
        block = descriptors[0]
        R, depth = block.shape
        CH = 2 if R % 32 == 0 else 1
        CR = R // CH
        share = H * R
        out = pltpu.VMEM((n - 1, 1, share), jnp.float32)
        vmem = pl.BlockSpec(memory_space=pltpu.VMEM)
        lo, se, norms = pl.pallas_call(
            functools.partial(kernel, n, D, H, CH),
            out_shape=(out, out, pltpu.VMEM((1, share), jnp.float32)),
            in_specs=[pl.BlockSpec(memory_space=pltpu.HBM)],
            out_specs=(vmem, vmem, vmem),
            scratch_shapes=[
                pltpu.VMEM((R, depth), jnp.bfloat16),
                pltpu.VMEM((T + 1, R, depth), jnp.bfloat16),
                pltpu.VMEM((D * share, depth), jnp.bfloat16),
                pltpu.VMEM((D * share, depth), jnp.bfloat16),
                pltpu.VMEM((D * share, 128), jnp.float32),
                pltpu.VMEM((T, 8, D * share), jnp.float32),
                pltpu.VMEM((T, 8, D * share), jnp.float32),
                pltpu.VMEM((T, D, 2, share), jnp.float32),
                pltpu.VMEM((T, D * H, 2, share), jnp.float32),
                pltpu.VMEM((T + 1, CH, 2, CR), jnp.float32),
                pltpu.VMEM((T, H, CH, 2, CR), jnp.float32),
                pltpu.SemaphoreType.DMA,
                pltpu.SemaphoreType.REGULAR((T,)),
                pltpu.SemaphoreType.REGULAR((max(D - 1, 1),)),
                pltpu.SemaphoreType.DMA((T, CH)),
                pltpu.SemaphoreType.DMA((T, CH)),
                pltpu.SemaphoreType.DMA,
                pltpu.SemaphoreType.DMA,
                pltpu.SemaphoreType.DMA((D * H, CH)),
                pltpu.SemaphoreType.DMA((D * H, CH)),
                pltpu.SemaphoreType.DMA((T, D * H)),
                pltpu.SemaphoreType.DMA((T, D * H)),
                pltpu.SemaphoreType.DMA((T + 1, H, CH)),
                pltpu.SemaphoreType.DMA((T, H, CH)),
            ],
            compiler_params=pltpu.CompilerParams(collective_id=0, has_side_effects=True),
        )(block)
        return norms + lo, norms + se

    in_specs = (P(("groups", "blk"), ("desc", "half"), None),)
    out_specs = (P(None, ("groups", "blk"), "desc"), P(None, ("groups", "blk"), "desc"))
    return jax.shard_map(
        per_device, mesh=mesh, in_specs=in_specs, out_specs=out_specs, check_vma=False
    )
```

```python
import functools

import jax
import jax.numpy as jnp
from jax import lax
from jax.experimental import pallas as pl
from jax.experimental.pallas import tpu as pltpu
from jax.sharding import PartitionSpec as P

MESH = pl.DeviceIdType.MESH


def combine(lo_a, se_a, lo_b, se_b):
    return (
        jnp.minimum(lo_a, lo_b),
        jnp.minimum(jnp.maximum(lo_a, lo_b), jnp.minimum(se_a, se_b)),
    )


def nt_dot(a, b):
    return lax.dot_general(a, b, (((1,), (1,)), ((), ())), preferred_element_type=jnp.float32)


def fold(part, norms, lo, se):
    wide = part.shape[1] // norms.shape[1]
    kept = [(lo, se), None]
    for r in range(part.shape[0] // 8):
        rows = slice(8 * r, 8 * r + 8)
        value = part[rows] + jnp.concatenate([norms[rows]] * wide, axis=1)
        if kept[r % 2] is None:
            kept[r % 2] = (value, jnp.full_like(value, jnp.inf))
        else:
            lo, se = kept[r % 2]
            kept[r % 2] = (jnp.minimum(lo, value), jnp.minimum(se, jnp.maximum(lo, value)))
    if kept[1] is None:
        return kept[0]
    return combine(*kept[0], *kept[1])


def across_rows(lo, se):
    for turn in (4, 2, 1):
        lo, se = combine(lo, se, pltpu.roll(lo, turn, 0), pltpu.roll(se, turn, 0))
    return lo[0:1], se[0:1]


def kernel(
    n, D, H, CH, x_hbm, best_ref, second_ref, norm_ref,
    x_ref, buf, q, q2, sn, low, sec, mine, inbox, turned, returned,
    x_sem, go, go_q, z_send, z_recv, y_send, y_recv, q_send, q_recv, p_send, p_recv, m_send, m_recv,
):
    R = x_hbm.shape[0]
    load = pltpu.make_async_copy(x_hbm, x_ref, x_sem)
    load.start()
    CR = R // CH
    share = H * R
    Q = D * share
    TQ = min(256, share)
    T = n // 2
    i = lax.axis_index("blk")
    d = lax.axis_index("desc")
    h = lax.axis_index("half")
    inf = functools.partial(jnp.full, fill_value=jnp.inf, dtype=jnp.float32)
    others = [(dd, hh) for dd in range(D) for hh in range(H) if (dd, hh) != (0, 0)]

    if n % 2 == 0:
        hosts_tie = (i < T) == (lax.rem(lax.rem(i, T), 2) == 0)
    else:
        hosts_tie = i >= 0

    def hosting(s):
        return (2 * s != n) | hosts_tie

    def visiting(s):
        if n % 2 == 0:
            return (2 * s != n) | jnp.logical_not(hosts_tie)
        return 2 * s != n

    def guest_of(s):
        return lax.rem(i - s + n, n)

    def host_of(s):
        return lax.rem(i + s, n)

    def peer(dd, hh):
        return {"desc": lax.rem(d + dd, D), "half": lax.rem(h + hh, H)}

    def rows_of(d_at, h_at):
        return pl.ds(pl.multiple_of((d_at * H + h_at) * R, R), R)

    def chunk(c):
        return pl.ds(pl.multiple_of(c * CR, CR), CR)

    barrier = pltpu.get_barrier_semaphore()

    def greet(s, met):
        for active, at in ((visiting(s), host_of(s)), (hosting(s), guest_of(s))):
            @pl.when(active & (i < at))
            def _():
                pl.semaphore_signal(barrier, inc=1, device_id={"blk": at}, device_id_type=MESH)

            met = met + jnp.where(active & (at < i), 1, 0)
        return met

    met = lax.fori_loop(1, T + 1, greet, jnp.int32(0))
    for dd in range(1, D):
        @pl.when(d + dd < D)
        def _():
            pl.semaphore_signal(barrier, inc=1, device_id={"desc": d + dd}, device_id_type=MESH)
    for hh in range(1, H):
        pl.semaphore_signal(barrier, inc=1, device_id=peer(0, hh), device_id_type=MESH)
    straight = D > 1 and H > 1
    if straight:
        for dd in range(1, D):
            @pl.when((d + dd < D) & (h == H - 1))
            def _():
                pl.semaphore_signal(
                    barrier, inc=1, device_id={"desc": d + dd, "half": 0}, device_id_type=MESH
                )

        met = met + jnp.where(h == 0, d, 0)
    pl.semaphore_wait(barrier, H - 1 + d + met)

    def invite(s, carry):
        at = guest_of(s)

        @pl.when(hosting(s) & (at < i))
        def _():
            pl.semaphore_signal(go.at[s - 1], inc=1, device_id={"blk": at}, device_id_type=MESH)

        return carry

    lax.fori_loop(1, T + 1, invite, 0)
    for dd in range(1, D):
        @pl.when(d >= dd)
        def _():
            pl.semaphore_signal(
                go_q.at[dd - 1], inc=1, device_id={"desc": d - dd}, device_id_type=MESH
            )

    detour = n % 2 == 0 and D > 1 and H > 1 and CH == 2
    gains = (i == 0) & (d == 0) & (h == H - 1) if detour else i < 0

    def keeps(s, c, guest):
        if not detour:
            return i >= 0
        elsewhere = (d != 1) | (h != 0) | (i != (T if guest else 0))
        return (s != T) | (c != CH - 1) | elsewhere

    def move(s, c):
        return pltpu.make_async_remote_copy(
            src_ref=x_ref.at[chunk(c)], dst_ref=buf.at[s - 1, chunk(c)],
            send_sem=z_send.at[s - 1, c], recv_sem=z_recv.at[s - 1, c],
            device_id={"blk": host_of(s)}, device_id_type=MESH,
        )

    mine_rows = rows_of(d, h)

    def part_of(d_at, h_at, c):
        return pl.ds(pl.multiple_of((d_at * H + h_at) * R + c * CR, CR), CR)

    def query_copy(dd, hh, c):
        return pltpu.make_async_remote_copy(
            src_ref=x_ref.at[chunk(c)], dst_ref=q.at[part_of(d, h, c)],
            send_sem=q_send.at[dd * H + hh, c], recv_sem=q_recv.at[dd * H + hh, c],
            device_id=peer(dd, hh), device_id_type=MESH,
        )

    def query_relay(dd, hh, c):
        rows = part_of(lax.rem(d + D - dd, D), h, c)
        return pltpu.make_async_remote_copy(
            src_ref=q.at[rows], dst_ref=q.at[rows],
            send_sem=q_send.at[dd * H + hh, c], recv_sem=q_recv.at[dd * H + hh, c],
            device_id=peer(0, hh), device_id_type=MESH,
        )

    def straight_copy(dd):
        at = dd * H + H - 1
        return pltpu.make_async_remote_copy(
            src_ref=x_ref.at[chunk(0)], dst_ref=q.at[part_of(d, 0, 0)],
            send_sem=q_send.at[at, 0], recv_sem=q_recv.at[at, 0],
            device_id={"desc": lax.rem(d + dd, D), "half": H - 1}, device_id_type=MESH,
        )

    def detour_copy():
        return pltpu.make_async_remote_copy(
            src_ref=q.at[part_of(1, 0, CH - 1)], dst_ref=buf.at[T, chunk(0)],
            send_sem=y_send, recv_sem=y_recv,
            device_id={"blk": i - T, "half": H - 1}, device_id_type=MESH,
        )

    load.wait()

    def move_down(s, carry):
        for c in range(CH):
            @pl.when(visiting(s) & (host_of(s) < i) & keeps(s, c, True))
            def _():
                move(s, c).start()

        return carry

    lax.fori_loop(1, T + 1, move_down, 0)
    for hh in range(1, H):
        for c in range(CH):
            query_copy(0, hh, c).start()
    for dd in range(1, D):
        @pl.when(d + dd < D)
        def _():
            pl.semaphore_wait(go_q.at[dd - 1], 1)

        for c in reversed(range(CH)):
            if straight and c == 0:
                @pl.when(h == 0)
                def _():
                    straight_copy(dd).start()

            query_copy(dd, 0, c).start()

    def widen(rows):
        wide = q[rows, :].astype(jnp.float32)
        q2[rows, :] = (wide * -2.0).astype(jnp.bfloat16)
        sn[rows, :] = jnp.broadcast_to(jnp.sum(wide * wide, axis=1, keepdims=True), (R, 128))

    q[mine_rows, :] = x_ref[...]
    widen(mine_rows)

    def move_up(s, carry):
        @pl.when(visiting(s) & (host_of(s) > i))
        def _():
            pl.semaphore_wait(go.at[s - 1], 1)
            for c in range(CH):
                move(s, c).start()

        return carry

    lax.fori_loop(1, T + 1, move_up, 0)

    def from_peer(dd, hh):
        return rows_of(lax.rem(d + D - dd, D), lax.rem(h + H - hh, H))

    for hh in range(1, H):
        for c in range(CH):
            query_copy(0, hh, c).wait_recv()
        widen(from_peer(0, hh))
    own = q[pl.ds(pl.multiple_of(d * share, share), share), :].astype(jnp.float32)
    square = own * own
    head = square.astype(jnp.bfloat16)
    tail = (square - head.astype(jnp.float32)).astype(jnp.bfloat16)
    ones = jnp.ones((8, q.shape[1]), jnp.bfloat16)
    norm_ref[...] = (nt_dot(ones, head) + nt_dot(ones, tail))[0:1]
    low[...] = inf(low.shape)
    sec[...] = inf(sec.shape)
    for dd in range(1, D):
        for c in reversed(range(CH)):
            query_copy(dd, 0, c).wait_recv()
            if detour and c == CH - 1 and dd == D - 1:
                @pl.when((i == T) & (d == 0) & (h == 0))
                def _():
                    detour_copy().start()
            for hh in range(1, H):
                if straight and (hh, c) == (H - 1, 0):
                    @pl.when(h != 0)
                    def _():
                        query_relay(dd, hh, c).start()
                else:
                    query_relay(dd, hh, c).start()
        widen(from_peer(dd, 0))
    for dd in range(1, D):
        for hh in range(1, H):
            for c in range(CH):
                query_copy(dd, hh, c).wait_recv()
            widen(from_peer(dd, hh))

    def result_copy(s, dd, hh):
        return pltpu.make_async_remote_copy(
            src_ref=mine.at[s - 1, lax.rem(d + dd, D)], dst_ref=inbox.at[s - 1, dd * H + hh],
            send_sem=p_send.at[s - 1, dd * H + hh], recv_sem=p_recv.at[s - 1, dd * H + hh],
            device_id=peer(dd, hh), device_id_type=MESH,
        )

    def return_copy(s, hh, c):
        return pltpu.make_async_remote_copy(
            src_ref=turned.at[s - 1, c], dst_ref=returned.at[s - 1, hh, c],
            send_sem=m_send.at[s - 1, hh, c], recv_sem=m_recv.at[s - 1, hh, c],
            device_id={"blk": guest_of(s), "half": lax.rem(h + hh, H)}, device_id_type=MESH,
        )

    def detour_return(hh):
        return pltpu.make_async_remote_copy(
            src_ref=turned.at[T, 0], dst_ref=returned.at[T - 1, hh, CH - 1],
            send_sem=m_send.at[T, hh, 0], recv_sem=m_recv.at[T - 1, hh, CH - 1],
            device_id={"blk": i + T, "desc": 1, "half": hh},
            device_id_type=MESH,
        )

    def host_side(s, at, c):
        piece = buf[at, chunk(c), :]
        wide = piece.astype(jnp.float32)
        norms = jnp.broadcast_to(jnp.sum(wide * wide, axis=1, keepdims=True), (CR, 128))
        for t in range(Q // TQ):
            lanes = slice(t * TQ, (t + 1) * TQ)
            lo, se = low[s - 1, :, lanes], sec[s - 1, :, lanes]
            lo, se = fold(nt_dot(piece, q2[lanes, :]), norms, lo, se)
            low[s - 1, :, lanes] = lo
            sec[s - 1, :, lanes] = se

    def host_close(s, at, c):
        piece = buf[at, chunk(c), :]
        wide = piece.astype(jnp.float32)
        norms = jnp.broadcast_to(jnp.sum(wide * wide, axis=1, keepdims=True), (CR, 128))

        def column(dd, carry):
            t = lax.rem(d + dd, D)
            for u in range(share // TQ):
                lanes = pl.ds(pl.multiple_of(t * share + u * TQ, TQ), TQ)
                lo, se = low[s - 1, :, lanes], sec[s - 1, :, lanes]
                lo, se = across_rows(*fold(nt_dot(piece, q2[lanes, :]), norms, lo, se))
                mine[s - 1, t, 0:1, u * TQ : (u + 1) * TQ] = lo
                mine[s - 1, t, 1:2, u * TQ : (u + 1) * TQ] = se

            @pl.when(dd < D)
            def _():
                for hh in range(H):
                    result_copy(s, dd, hh).start()

            @pl.when(dd == D)
            def _():
                for hh in range(1, H):
                    result_copy(s, 0, hh).start()

            return carry

        lax.fori_loop(1, D + 1, column, 0)

    def host_send(s):
        for t in range(D):
            lanes = slice(t * share, (t + 1) * share)
            lo, se = across_rows(low[s - 1, :, lanes], sec[s - 1, :, lanes])
            mine[s - 1, t, 0:1, :] = lo
            mine[s - 1, t, 1:2, :] = se
        for dd, hh in reversed(others):
            result_copy(s, dd, hh).start()

    def guest_side(at, rows, width):
        piece = buf[at, rows, :]
        lo, se = inf((8, width)), inf((8, width))
        for t in range(Q // TQ):
            rows = slice(t * TQ, (t + 1) * TQ)
            lo, se = fold(nt_dot(q2[rows, :], piece), sn[rows, :], lo, se)
        return across_rows(lo, se)

    def guest_chunk(s, at, c):
        lo, se = guest_side(at, chunk(c), CR)
        turned[at, c, 0:1, :] = lo
        turned[at, c, 1:2, :] = se

        @pl.when(at < T)
        def _():
            for hh in range(H):
                return_copy(s, hh, c).start()

        if detour:
            @pl.when(at == T)
            def _():
                for hh in range(H):
                    detour_return(hh).start()

    def guest_whole(s):
        lo, se = guest_side(s - 1, slice(0, R), R)
        for c in range(CH):
            lanes = slice(c * CR, (c + 1) * CR)
            turned[s - 1, c, 0:1, :] = lo[:, lanes]
            turned[s - 1, c, 1:2, :] = se[:, lanes]
            for hh in range(H):
                return_copy(s, hh, c).start()

    def turn_of(k):
        rest = (T - 1) * CH
        upper = (2 * i >= n) & (k > 0)
        far = upper & (k <= rest)
        s = jnp.where(upper, jnp.where(far, 1 + (k + CH - 1) // CH, 1), k // CH + 1)
        c = jnp.where(upper, jnp.where(far, lax.rem(k + CH - 1, CH), k - rest), lax.rem(k, CH))
        return s, c

    items = T * CH + (1 if detour else 0)

    def meet(k, carry):
        s, c = turn_of(k)
        at = s - 1
        comes = hosting(s) & keeps(s, c, False)
        closes = (c == CH - 1) & jnp.logical_not(gains & (s == T))
        lost, extra = i < 0, i < 0
        if detour:
            extra = k == T * CH
            s, c, at = jnp.where(extra, T, s), jnp.where(extra, 0, c), jnp.where(extra, T, at)
            comes = jnp.where(extra, gains, comes)
            lost = jnp.logical_not(keeps(s, CH - 1, False))
            closes = extra | closes | (lost & (c == CH - 2))

        @pl.when(comes & (at < T))
        def _():
            move(s, c).wait_recv()

        if detour:
            @pl.when(comes & (at == T))
            def _():
                detour_copy().wait_recv()

        lower = 2 * i < n

        last_far = closes & (s == T) & jnp.logical_not(lower) & (T > 1)

        @pl.when(comes & jnp.logical_not(lower) & jnp.logical_not(last_far))
        def _():
            host_side(s, at, c)
            guest_chunk(s, at, c)

            @pl.when(closes)
            def _():
                host_send(s)

        @pl.when(comes & last_far)
        def _():
            guest_chunk(s, at, c)

        @pl.when(comes & lower)
        def _():
            travels = closes & (d > 0)

            @pl.when(travels)
            def _():
                host_close(s, at, c)

            @pl.when(jnp.logical_not(travels))
            def _():
                host_side(s, at, c)

            @pl.when(closes & jnp.logical_not(travels))
            def _():
                host_send(s)

            whole = closes & (extra | jnp.logical_not(lost))

            @pl.when(whole & ((d == 0) | (s == T)))
            def _():
                guest_whole(s)

            @pl.when(extra | (closes & lost))
            def _():
                guest_chunk(s, at, c)

        return carry

    lax.fori_loop(0, items, meet, 0)

    if T > 1:
        @pl.when((2 * i >= n) & hosting(T))
        def _():
            host_side(T, T - 1, CH - 1)
            host_send(T)

    def put_off(s, carry):
        @pl.when((2 * i < n) & (d > 0) & hosting(s))
        def _():
            guest_whole(s)

        return carry

    lax.fori_loop(1, T, put_off, 0)

    def sent(s, carry):
        for c in range(CH):
            @pl.when(visiting(s) & keeps(s, c, True))
            def _():
                move(s, c).wait_send()

        return carry

    lax.fori_loop(1, T + 1, sent, 0)
    if detour:
        @pl.when((i == T) & (d == 0) & (h == 0))
        def _():
            detour_copy().wait_send()
    for c in range(CH):
        for dd in range(1, D):
            query_copy(dd, 0, c).wait_send()
            for hh in range(1, H):
                query_relay(dd, hh, c).wait_send()
        for hh in range(1, H):
            query_copy(0, hh, c).wait_send()

    def sent_results(s, carry):
        @pl.when(hosting(s))
        def _():
            for dd, hh in others:
                result_copy(s, dd, hh).wait_send()

        for c in range(CH):
            @pl.when(hosting(s) & keeps(s, c, False))
            def _():
                for hh in range(H):
                    return_copy(s, hh, c).wait_send()

        return carry

    lax.fori_loop(1, T + 1, sent_results, 0)
    if detour:
        @pl.when(gains)
        def _():
            for hh in range(H):
                detour_return(hh).wait_send()

    def finish(s, carry):
        @pl.when(visiting(s))
        def _():
            for hh in range(H):
                for c in range(CH):
                    return_copy(s, hh, c).wait_recv()
            for hh in range(H):
                for c in range(CH):
                    at = lax.rem(h + H - hh, H) * CH + c
                    lanes = pl.ds(pl.multiple_of(at * CR, CR), CR)
                    best_ref[n - s - 1, :, lanes] = returned[s - 1, hh, c, 0:1, :]
                    second_ref[n - s - 1, :, lanes] = returned[s - 1, hh, c, 1:2, :]

        @pl.when(hosting(s))
        def _():
            lo, se = mine[s - 1, d, 0:1, :], mine[s - 1, d, 1:2, :]
            for dd, hh in others:
                result_copy(s, dd, hh).wait_recv()
                at = dd * H + hh
                lo, se = combine(lo, se, inbox[s - 1, at, 0:1, :], inbox[s - 1, at, 1:2, :])
            best_ref[s - 1] = lo
            second_ref[s - 1] = se

        return carry

    lax.fori_loop(1, T + 1, finish, 0)


def solution(mesh):
    n, D, H = mesh.shape["blk"], mesh.shape["desc"], mesh.shape["half"]
    T = n // 2

    def per_device(descriptors):
        block = descriptors[0]
        R, depth = block.shape
        CH = 2 if R % 32 == 0 else 1
        CR = R // CH
        share = H * R
        out = pltpu.VMEM((n - 1, 1, share), jnp.float32)
        vmem = pl.BlockSpec(memory_space=pltpu.VMEM)
        lo, se, norms = pl.pallas_call(
            functools.partial(kernel, n, D, H, CH),
            out_shape=(out, out, pltpu.VMEM((1, share), jnp.float32)),
            in_specs=[pl.BlockSpec(memory_space=pltpu.HBM)],
            out_specs=(vmem, vmem, vmem),
            scratch_shapes=[
                pltpu.VMEM((R, depth), jnp.bfloat16),
                pltpu.VMEM((T + 1, R, depth), jnp.bfloat16),
                pltpu.VMEM((D * share, depth), jnp.bfloat16),
                pltpu.VMEM((D * share, depth), jnp.bfloat16),
                pltpu.VMEM((D * share, 128), jnp.float32),
                pltpu.VMEM((T, 8, D * share), jnp.float32),
                pltpu.VMEM((T, 8, D * share), jnp.float32),
                pltpu.VMEM((T, D, 2, share), jnp.float32),
                pltpu.VMEM((T, D * H, 2, share), jnp.float32),
                pltpu.VMEM((T + 1, CH, 2, CR), jnp.float32),
                pltpu.VMEM((T, H, CH, 2, CR), jnp.float32),
                pltpu.SemaphoreType.DMA,
                pltpu.SemaphoreType.REGULAR((T,)),
                pltpu.SemaphoreType.REGULAR((max(D - 1, 1),)),
                pltpu.SemaphoreType.DMA((T, CH)),
                pltpu.SemaphoreType.DMA((T, CH)),
                pltpu.SemaphoreType.DMA,
                pltpu.SemaphoreType.DMA,
                pltpu.SemaphoreType.DMA((D * H, CH)),
                pltpu.SemaphoreType.DMA((D * H, CH)),
                pltpu.SemaphoreType.DMA((T, D * H)),
                pltpu.SemaphoreType.DMA((T, D * H)),
                pltpu.SemaphoreType.DMA((T + 1, H, CH)),
                pltpu.SemaphoreType.DMA((T, H, CH)),
            ],
            compiler_params=pltpu.CompilerParams(collective_id=0, has_side_effects=True),
        )(block)
        return norms + lo, norms + se

    in_specs = (P(("groups", "blk"), ("desc", "half"), None),)
    out_specs = (P(None, ("groups", "blk"), "desc"), P(None, ("groups", "blk"), "desc"))
    return jax.shard_map(
        per_device, mesh=mesh, in_specs=in_specs, out_specs=out_specs, check_vma=False
    )
```

```python
import functools

import jax
import jax.numpy as jnp
from jax import lax
from jax.experimental import pallas as pl
from jax.experimental.pallas import tpu as pltpu
from jax.sharding import PartitionSpec as P

MESH = pl.DeviceIdType.MESH


def combine(lo_a, se_a, lo_b, se_b):
    return (
        jnp.minimum(lo_a, lo_b),
        jnp.minimum(jnp.maximum(lo_a, lo_b), jnp.minimum(se_a, se_b)),
    )


def nt_dot(a, b):
    return lax.dot_general(a, b, (((1,), (1,)), ((), ())), preferred_element_type=jnp.float32)


def fold(part, norms, lo, se):
    wide = part.shape[1] // norms.shape[1]
    kept = [(lo, se), None]
    for r in range(part.shape[0] // 8):
        rows = slice(8 * r, 8 * r + 8)
        value = part[rows] + jnp.concatenate([norms[rows]] * wide, axis=1)
        if kept[r % 2] is None:
            kept[r % 2] = (value, jnp.full_like(value, jnp.inf))
        else:
            lo, se = kept[r % 2]
            kept[r % 2] = (jnp.minimum(lo, value), jnp.minimum(se, jnp.maximum(lo, value)))
    if kept[1] is None:
        return kept[0]
    return combine(*kept[0], *kept[1])


def across_rows(lo, se):
    for turn in (4, 2, 1):
        lo, se = combine(lo, se, pltpu.roll(lo, turn, 0), pltpu.roll(se, turn, 0))
    return lo[0:1], se[0:1]


def kernel(
    n, D, H, CH, x_hbm, best_ref, second_ref, norm_ref,
    x_ref, buf, q, q2, sn, low, sec, mine, inbox, turned, returned,
    x_sem, go, go_q, z_send, z_recv, y_send, y_recv, q_send, q_recv, p_send, p_recv, m_send, m_recv,
):
    R = x_hbm.shape[0]
    load = pltpu.make_async_copy(x_hbm, x_ref, x_sem)
    load.start()
    CR = R // CH
    share = H * R
    Q = D * share
    TQ = min(256, share)
    T = n // 2
    i = lax.axis_index("blk")
    d = lax.axis_index("desc")
    h = lax.axis_index("half")
    inf = functools.partial(jnp.full, fill_value=jnp.inf, dtype=jnp.float32)
    others = [(dd, hh) for dd in range(D) for hh in range(H) if (dd, hh) != (0, 0)]

    if n % 2 == 0:
        hosts_tie = (i < T) == (lax.rem(lax.rem(i, T), 2) == 0)
    else:
        hosts_tie = i >= 0

    def hosting(s):
        return (2 * s != n) | hosts_tie

    def visiting(s):
        if n % 2 == 0:
            return (2 * s != n) | jnp.logical_not(hosts_tie)
        return 2 * s != n

    def guest_of(s):
        return lax.rem(i - s + n, n)

    def host_of(s):
        return lax.rem(i + s, n)

    def peer(dd, hh):
        return {"desc": lax.rem(d + dd, D), "half": lax.rem(h + hh, H)}

    def rows_of(d_at, h_at):
        return pl.ds(pl.multiple_of((d_at * H + h_at) * R, R), R)

    def chunk(c):
        return pl.ds(pl.multiple_of(c * CR, CR), CR)

    barrier = pltpu.get_barrier_semaphore()

    def greet(s, met):
        for active, at in ((visiting(s), host_of(s)), (hosting(s), guest_of(s))):
            @pl.when(active & (i < at))
            def _():
                pl.semaphore_signal(barrier, inc=1, device_id={"blk": at}, device_id_type=MESH)

            met = met + jnp.where(active & (at < i), 1, 0)
        return met

    met = lax.fori_loop(1, T + 1, greet, jnp.int32(0))
    for dd in range(1, D):
        @pl.when(d + dd < D)
        def _():
            pl.semaphore_signal(barrier, inc=1, device_id={"desc": d + dd}, device_id_type=MESH)
    for hh in range(1, H):
        pl.semaphore_signal(barrier, inc=1, device_id=peer(0, hh), device_id_type=MESH)
    straight = D > 1 and H > 1
    if straight:
        for dd in range(1, D):
            @pl.when((d + dd < D) & (h == H - 1))
            def _():
                pl.semaphore_signal(
                    barrier, inc=1, device_id={"desc": d + dd, "half": 0}, device_id_type=MESH
                )

        met = met + jnp.where(h == 0, d, 0)
    pl.semaphore_wait(barrier, H - 1 + d + met)

    def invite(s, carry):
        at = guest_of(s)

        @pl.when(hosting(s) & (at < i))
        def _():
            pl.semaphore_signal(go.at[s - 1], inc=1, device_id={"blk": at}, device_id_type=MESH)

        return carry

    lax.fori_loop(1, T + 1, invite, 0)
    for dd in range(1, D):
        @pl.when(d >= dd)
        def _():
            pl.semaphore_signal(
                go_q.at[dd - 1], inc=1, device_id={"desc": d - dd}, device_id_type=MESH
            )

    detour = n % 2 == 0 and D > 1 and H > 1 and CH == 2
    gains = (i == 0) & (d == 0) & (h == H - 1) if detour else i < 0

    def keeps(s, c, guest):
        if not detour:
            return i >= 0
        elsewhere = (d != 1) | (h != 0) | (i != (T if guest else 0))
        return (s != T) | (c != CH - 1) | elsewhere

    def move(s, c):
        return pltpu.make_async_remote_copy(
            src_ref=x_ref.at[chunk(c)], dst_ref=buf.at[s - 1, chunk(c)],
            send_sem=z_send.at[s - 1, c], recv_sem=z_recv.at[s - 1, c],
            device_id={"blk": host_of(s)}, device_id_type=MESH,
        )

    mine_rows = rows_of(d, h)

    def part_of(d_at, h_at, c):
        return pl.ds(pl.multiple_of((d_at * H + h_at) * R + c * CR, CR), CR)

    def query_copy(dd, hh, c):
        return pltpu.make_async_remote_copy(
            src_ref=x_ref.at[chunk(c)], dst_ref=q.at[part_of(d, h, c)],
            send_sem=q_send.at[dd * H + hh, c], recv_sem=q_recv.at[dd * H + hh, c],
            device_id=peer(dd, hh), device_id_type=MESH,
        )

    def query_relay(dd, hh, c):
        rows = part_of(lax.rem(d + D - dd, D), h, c)
        return pltpu.make_async_remote_copy(
            src_ref=q.at[rows], dst_ref=q.at[rows],
            send_sem=q_send.at[dd * H + hh, c], recv_sem=q_recv.at[dd * H + hh, c],
            device_id=peer(0, hh), device_id_type=MESH,
        )

    def straight_copy(dd):
        at = dd * H + H - 1
        return pltpu.make_async_remote_copy(
            src_ref=x_ref.at[chunk(0)], dst_ref=q.at[part_of(d, 0, 0)],
            send_sem=q_send.at[at, 0], recv_sem=q_recv.at[at, 0],
            device_id={"desc": lax.rem(d + dd, D), "half": H - 1}, device_id_type=MESH,
        )

    def detour_copy():
        return pltpu.make_async_remote_copy(
            src_ref=q.at[part_of(1, 0, CH - 1)], dst_ref=buf.at[T, chunk(0)],
            send_sem=y_send, recv_sem=y_recv,
            device_id={"blk": i - T, "half": H - 1}, device_id_type=MESH,
        )

    load.wait()

    yields = (i == T) & (d == 1) & (h == H - 1) if detour else i < 0

    def move_down(s, carry, again=False):
        for c in range(CH):
            now = yields & (c == CH - 1)
            now = now if again else jnp.logical_not(now)

            @pl.when(now & visiting(s) & (host_of(s) < i) & keeps(s, c, True))
            def _():
                move(s, c).start()

        return carry

    lax.fori_loop(1, T + 1, move_down, 0)
    for hh in range(1, H):
        for c in range(CH):
            query_copy(0, hh, c).start()
    for dd in range(1, D):
        @pl.when(d + dd < D)
        def _():
            pl.semaphore_wait(go_q.at[dd - 1], 1)

        for c in reversed(range(CH)):
            if straight and c == 0:
                @pl.when(h == 0)
                def _():
                    straight_copy(dd).start()

            query_copy(dd, 0, c).start()

    def widen(rows):
        wide = q[rows, :].astype(jnp.float32)
        q2[rows, :] = (wide * -2.0).astype(jnp.bfloat16)
        sn[rows, :] = jnp.broadcast_to(jnp.sum(wide * wide, axis=1, keepdims=True), (R, 128))

    q[mine_rows, :] = x_ref[...]
    widen(mine_rows)

    def move_up(s, carry):
        @pl.when(visiting(s) & (host_of(s) > i))
        def _():
            pl.semaphore_wait(go.at[s - 1], 1)
            for c in range(CH):
                move(s, c).start()

        return carry

    lax.fori_loop(1, T + 1, move_up, 0)

    def from_peer(dd, hh):
        return rows_of(lax.rem(d + D - dd, D), lax.rem(h + H - hh, H))

    for hh in range(1, H):
        for c in range(CH):
            query_copy(0, hh, c).wait_recv()
        if hh == 1:
            lax.fori_loop(1, T + 1, functools.partial(move_down, again=True), 0)
        widen(from_peer(0, hh))
    own = q[pl.ds(pl.multiple_of(d * share, share), share), :].astype(jnp.float32)
    square = own * own
    head = square.astype(jnp.bfloat16)
    tail = (square - head.astype(jnp.float32)).astype(jnp.bfloat16)
    ones = jnp.ones((8, q.shape[1]), jnp.bfloat16)
    norm_ref[...] = (nt_dot(ones, head) + nt_dot(ones, tail))[0:1]
    low[...] = inf(low.shape)
    sec[...] = inf(sec.shape)
    for dd in range(1, D):
        for c in reversed(range(CH)):
            query_copy(dd, 0, c).wait_recv()
            if detour and c == CH - 1 and dd == D - 1:
                @pl.when((i == T) & (d == 0) & (h == 0))
                def _():
                    detour_copy().start()
            for hh in range(1, H):
                if straight and (hh, c) == (H - 1, 0):
                    @pl.when(h != 0)
                    def _():
                        query_relay(dd, hh, c).start()
                else:
                    query_relay(dd, hh, c).start()
        widen(from_peer(dd, 0))
    for dd in range(1, D):
        for hh in range(1, H):
            for c in range(CH):
                query_copy(dd, hh, c).wait_recv()
            widen(from_peer(dd, hh))

    def result_copy(s, dd, hh):
        return pltpu.make_async_remote_copy(
            src_ref=mine.at[s - 1, lax.rem(d + dd, D)], dst_ref=inbox.at[s - 1, dd * H + hh],
            send_sem=p_send.at[s - 1, dd * H + hh], recv_sem=p_recv.at[s - 1, dd * H + hh],
            device_id=peer(dd, hh), device_id_type=MESH,
        )

    def return_copy(s, hh, c):
        return pltpu.make_async_remote_copy(
            src_ref=turned.at[s - 1, c], dst_ref=returned.at[s - 1, hh, c],
            send_sem=m_send.at[s - 1, hh, c], recv_sem=m_recv.at[s - 1, hh, c],
            device_id={"blk": guest_of(s), "half": lax.rem(h + hh, H)}, device_id_type=MESH,
        )

    def detour_return(hh):
        return pltpu.make_async_remote_copy(
            src_ref=turned.at[T, 0], dst_ref=returned.at[T - 1, hh, CH - 1],
            send_sem=m_send.at[T, hh, 0], recv_sem=m_recv.at[T - 1, hh, CH - 1],
            device_id={"blk": i + T, "desc": 1, "half": hh},
            device_id_type=MESH,
        )

    def host_side(s, at, c):
        piece = buf[at, chunk(c), :]
        wide = piece.astype(jnp.float32)
        norms = jnp.broadcast_to(jnp.sum(wide * wide, axis=1, keepdims=True), (CR, 128))
        for t in range(Q // TQ):
            lanes = slice(t * TQ, (t + 1) * TQ)
            lo, se = low[s - 1, :, lanes], sec[s - 1, :, lanes]
            lo, se = fold(nt_dot(piece, q2[lanes, :]), norms, lo, se)
            low[s - 1, :, lanes] = lo
            sec[s - 1, :, lanes] = se

    def host_close(s, at, c):
        piece = buf[at, chunk(c), :]
        wide = piece.astype(jnp.float32)
        norms = jnp.broadcast_to(jnp.sum(wide * wide, axis=1, keepdims=True), (CR, 128))

        def column(dd, carry):
            t = lax.rem(d + dd, D)
            for u in range(share // TQ):
                lanes = pl.ds(pl.multiple_of(t * share + u * TQ, TQ), TQ)
                lo, se = low[s - 1, :, lanes], sec[s - 1, :, lanes]
                lo, se = across_rows(*fold(nt_dot(piece, q2[lanes, :]), norms, lo, se))
                mine[s - 1, t, 0:1, u * TQ : (u + 1) * TQ] = lo
                mine[s - 1, t, 1:2, u * TQ : (u + 1) * TQ] = se

            @pl.when(dd < D)
            def _():
                for hh in range(H):
                    result_copy(s, dd, hh).start()

            @pl.when(dd == D)
            def _():
                for hh in range(1, H):
                    result_copy(s, 0, hh).start()

            return carry

        lax.fori_loop(1, D + 1, column, 0)

    def host_send(s):
        for t in range(D):
            lanes = slice(t * share, (t + 1) * share)
            lo, se = across_rows(low[s - 1, :, lanes], sec[s - 1, :, lanes])
            mine[s - 1, t, 0:1, :] = lo
            mine[s - 1, t, 1:2, :] = se
        for dd, hh in reversed(others):
            result_copy(s, dd, hh).start()

    def guest_side(at, rows, width):
        piece = buf[at, rows, :]
        lo, se = inf((8, width)), inf((8, width))
        for t in range(Q // TQ):
            rows = slice(t * TQ, (t + 1) * TQ)
            lo, se = fold(nt_dot(q2[rows, :], piece), sn[rows, :], lo, se)
        return across_rows(lo, se)

    def guest_chunk(s, at, c):
        lo, se = guest_side(at, chunk(c), CR)
        turned[at, c, 0:1, :] = lo
        turned[at, c, 1:2, :] = se

        @pl.when(at < T)
        def _():
            for hh in range(H):
                return_copy(s, hh, c).start()

        if detour:
            @pl.when(at == T)
            def _():
                for hh in range(H):
                    detour_return(hh).start()

    def guest_whole(s):
        lo, se = guest_side(s - 1, slice(0, R), R)
        for c in range(CH):
            lanes = slice(c * CR, (c + 1) * CR)
            turned[s - 1, c, 0:1, :] = lo[:, lanes]
            turned[s - 1, c, 1:2, :] = se[:, lanes]
            for hh in range(H):
                return_copy(s, hh, c).start()

    def turn_of(k):
        rest = (T - 1) * CH
        upper = (2 * i >= n) & (k > 0)
        far = upper & (k <= rest)
        s = jnp.where(upper, jnp.where(far, 1 + (k + CH - 1) // CH, 1), k // CH + 1)
        c = jnp.where(upper, jnp.where(far, lax.rem(k + CH - 1, CH), k - rest), lax.rem(k, CH))
        return s, c

    items = T * CH + (1 if detour else 0)

    def meet(k, carry):
        s, c = turn_of(k)
        at = s - 1
        comes = hosting(s) & keeps(s, c, False)
        closes = (c == CH - 1) & jnp.logical_not(gains & (s == T))
        lost, extra = i < 0, i < 0
        if detour:
            extra = k == T * CH
            s, c, at = jnp.where(extra, T, s), jnp.where(extra, 0, c), jnp.where(extra, T, at)
            comes = jnp.where(extra, gains, comes)
            lost = jnp.logical_not(keeps(s, CH - 1, False))
            closes = extra | closes | (lost & (c == CH - 2))

        @pl.when(comes & (at < T))
        def _():
            move(s, c).wait_recv()

        if detour:
            @pl.when(comes & (at == T))
            def _():
                detour_copy().wait_recv()

        lower = 2 * i < n

        last_far = closes & (s == T) & jnp.logical_not(lower) & (T > 1)

        @pl.when(comes & jnp.logical_not(lower) & jnp.logical_not(last_far))
        def _():
            host_side(s, at, c)
            guest_chunk(s, at, c)

            @pl.when(closes)
            def _():
                host_send(s)

        @pl.when(comes & last_far)
        def _():
            guest_chunk(s, at, c)

        @pl.when(comes & lower)
        def _():
            travels = closes & (d > 0)

            @pl.when(travels)
            def _():
                host_close(s, at, c)

            @pl.when(jnp.logical_not(travels))
            def _():
                host_side(s, at, c)

            @pl.when(closes & jnp.logical_not(travels))
            def _():
                host_send(s)

            whole = closes & (extra | jnp.logical_not(lost))

            @pl.when(whole & ((d == 0) | (s == T)))
            def _():
                guest_whole(s)

            @pl.when(extra | (closes & lost))
            def _():
                guest_chunk(s, at, c)

        return carry

    lax.fori_loop(0, items, meet, 0)

    if T > 1:
        @pl.when((2 * i >= n) & hosting(T))
        def _():
            host_side(T, T - 1, CH - 1)
            host_send(T)

    def put_off(s, carry):
        @pl.when((2 * i < n) & (d > 0) & hosting(s))
        def _():
            guest_whole(s)

        return carry

    lax.fori_loop(1, T, put_off, 0)

    def sent(s, carry):
        for c in range(CH):
            @pl.when(visiting(s) & keeps(s, c, True))
            def _():
                move(s, c).wait_send()

        return carry

    lax.fori_loop(1, T + 1, sent, 0)
    if detour:
        @pl.when((i == T) & (d == 0) & (h == 0))
        def _():
            detour_copy().wait_send()
    for c in range(CH):
        for dd in range(1, D):
            query_copy(dd, 0, c).wait_send()
            for hh in range(1, H):
                query_relay(dd, hh, c).wait_send()
        for hh in range(1, H):
            query_copy(0, hh, c).wait_send()

    def sent_results(s, carry):
        @pl.when(hosting(s))
        def _():
            for dd, hh in others:
                result_copy(s, dd, hh).wait_send()

        for c in range(CH):
            @pl.when(hosting(s) & keeps(s, c, False))
            def _():
                for hh in range(H):
                    return_copy(s, hh, c).wait_send()

        return carry

    lax.fori_loop(1, T + 1, sent_results, 0)
    if detour:
        @pl.when(gains)
        def _():
            for hh in range(H):
                detour_return(hh).wait_send()

    def finish(s, carry):
        @pl.when(visiting(s))
        def _():
            for hh in range(H):
                for c in range(CH):
                    return_copy(s, hh, c).wait_recv()
            for hh in range(H):
                for c in range(CH):
                    at = lax.rem(h + H - hh, H) * CH + c
                    lanes = pl.ds(pl.multiple_of(at * CR, CR), CR)
                    best_ref[n - s - 1, :, lanes] = returned[s - 1, hh, c, 0:1, :]
                    second_ref[n - s - 1, :, lanes] = returned[s - 1, hh, c, 1:2, :]

        @pl.when(hosting(s))
        def _():
            lo, se = mine[s - 1, d, 0:1, :], mine[s - 1, d, 1:2, :]
            for dd, hh in others:
                result_copy(s, dd, hh).wait_recv()
                at = dd * H + hh
                lo, se = combine(lo, se, inbox[s - 1, at, 0:1, :], inbox[s - 1, at, 1:2, :])
            best_ref[s - 1] = lo
            second_ref[s - 1] = se

        return carry

    lax.fori_loop(1, T + 1, finish, 0)


def solution(mesh):
    n, D, H = mesh.shape["blk"], mesh.shape["desc"], mesh.shape["half"]
    T = n // 2

    def per_device(descriptors):
        block = descriptors[0]
        R, depth = block.shape
        CH = 2 if R % 32 == 0 else 1
        CR = R // CH
        share = H * R
        out = pltpu.VMEM((n - 1, 1, share), jnp.float32)
        vmem = pl.BlockSpec(memory_space=pltpu.VMEM)
        lo, se, norms = pl.pallas_call(
            functools.partial(kernel, n, D, H, CH),
            out_shape=(out, out, pltpu.VMEM((1, share), jnp.float32)),
            in_specs=[pl.BlockSpec(memory_space=pltpu.HBM)],
            out_specs=(vmem, vmem, vmem),
            scratch_shapes=[
                pltpu.VMEM((R, depth), jnp.bfloat16),
                pltpu.VMEM((T + 1, R, depth), jnp.bfloat16),
                pltpu.VMEM((D * share, depth), jnp.bfloat16),
                pltpu.VMEM((D * share, depth), jnp.bfloat16),
                pltpu.VMEM((D * share, 128), jnp.float32),
                pltpu.VMEM((T, 8, D * share), jnp.float32),
                pltpu.VMEM((T, 8, D * share), jnp.float32),
                pltpu.VMEM((T, D, 2, share), jnp.float32),
                pltpu.VMEM((T, D * H, 2, share), jnp.float32),
                pltpu.VMEM((T + 1, CH, 2, CR), jnp.float32),
                pltpu.VMEM((T, H, CH, 2, CR), jnp.float32),
                pltpu.SemaphoreType.DMA,
                pltpu.SemaphoreType.REGULAR((T,)),
                pltpu.SemaphoreType.REGULAR((max(D - 1, 1),)),
                pltpu.SemaphoreType.DMA((T, CH)),
                pltpu.SemaphoreType.DMA((T, CH)),
                pltpu.SemaphoreType.DMA,
                pltpu.SemaphoreType.DMA,
                pltpu.SemaphoreType.DMA((D * H, CH)),
                pltpu.SemaphoreType.DMA((D * H, CH)),
                pltpu.SemaphoreType.DMA((T, D * H)),
                pltpu.SemaphoreType.DMA((T, D * H)),
                pltpu.SemaphoreType.DMA((T + 1, H, CH)),
                pltpu.SemaphoreType.DMA((T, H, CH)),
            ],
            compiler_params=pltpu.CompilerParams(collective_id=0, has_side_effects=True),
        )(block)
        return norms + lo, norms + se

    in_specs = (P(("groups", "blk"), ("desc", "half"), None),)
    out_specs = (P(None, ("groups", "blk"), "desc"), P(None, ("groups", "blk"), "desc"))
    return jax.shard_map(
        per_device, mesh=mesh, in_specs=in_specs, out_specs=out_specs, check_vma=False
    )
```
